32 devices in a mesh: pitch: 4 (over x, core), span: 8 (over z, y).
Axes of the slice: x: 2, y: 2, z: 4, core: 2. Of those that a mesh axis runs over, the one named last changes fastest.
Arguments:
- residual: float32 [5, 4, 64, 1024], P(None, None, 'span', 'pitch'), may hold values from -0.6 to 0.6
- inverse_diagonal: float32 [5, 5, 4, 64, 1024], P(None, None, None, 'span', 'pitch'), may hold values from -0.1 to 1, as said below
- prior_increment: float32 [5, 4, 64, 1024], P(None, None, 'span', 'pitch'), may hold values from -3 to 3
- coupling: float32 [6, 5, 5], replicated, may hold values from -1 to 1
- characteristic: float32 [2, 2, 512, 5, 5], replicated, may hold values from -6 to 6
- cutoffs: int32 [2], replicated, may hold values from 128 to 512
Outputs:
- update: float32 [5, 4, 64, 1024], P(None, None, 'span', 'pitch')
The draws below stay inside these ranges and needn't reach their ends.
Inputs may be any that keep to these rules, and one draw needn't show every extreme that they name: `inverse_diagonal`: each cell's block is dominated by its diagonal; the sweeps' recurrences are stable.
All inputs are finite; a program needn't handle non-finite values.
Results may differ from the reference program's by a relative error of at most 0.0003.
Values sent between devices are 32-bit elements; how exact they have to be, the bound alone decides.
No kernel may reach another device: no remote copies, remote signals or barrier semaphores. Data moves between devices by JAX's collectives and lax.ppermute only.
A program may use at most 64 MiB of HBM per device.

```python
import jax
import jax.numpy as jnp
from jax import lax

VARIABLES = 5
NP = 1024
HARMONICS = 512
AXIAL = 4
SPANWISE_VOLUMES = 64


def draw_inverse_diagonal(key, part):
    first_key, interaction_seed, third_key = jax.random.split(jax.random.fold_in(key, 11), 3)
    shape = (VARIABLES, AXIAL, SPANWISE_VOLUMES, NP)
    spread = jax.random.uniform(first_key, shape, jnp.float32, 0.0, 0.004)
    relaxation_passes = jax.random.randint(interaction_seed, (2,), 0, SPANWISE_VOLUMES)
    spanwise_location = jnp.arange(SPANWISE_VOLUMES, dtype=jnp.int32)
    affected_volumes = jnp.any(spanwise_location[:, None] == relaxation_passes[None, :], axis=1)
    factor = jnp.where(affected_volumes, 0.75, 1.0).astype(jnp.float32)[None, None, :, None]
    diagonal = jnp.exp(-spread) * factor
    full_shape = (VARIABLES, VARIABLES, AXIAL, SPANWISE_VOLUMES, NP)
    offdiag = jnp.clip(0.03 * jax.random.normal(third_key, full_shape, jnp.float32), -0.1, 0.1)
    identity = jnp.eye(VARIABLES, dtype=jnp.float32)[:, :, None, None, None]
    return offdiag * (1.0 - identity) + identity * diagonal[:, None]


def draw_coupling(key, part):
    keys = jax.random.split(jax.random.fold_in(key, 23), 4)
    order = jax.random.permutation(keys[0], VARIABLES)
    slow = order < 3
    rates = jnp.where(slow, 0.998, 0.9).astype(jnp.float32)
    lower_part = jnp.tril(0.05 * jax.random.normal(keys[1], (VARIABLES, VARIABLES), jnp.float32), -1)
    upper_part = jnp.tril(0.05 * jax.random.normal(keys[2], (VARIABLES, VARIABLES), jnp.float32), -1)
    radial_lower = -(jnp.diag(rates) + lower_part)
    radial_upper = jnp.diag(rates) + upper_part
    others = jnp.clip(0.1 * jax.random.normal(keys[3], (4, VARIABLES, VARIABLES), jnp.float32), -0.4, 0.4)
    return jnp.concatenate([radial_lower[None], radial_upper[None], others], axis=0)


def block_scale(rng, shape, pieces, low, high):
    def one(position, parts):
        steps = jax.random.uniform(jax.random.fold_in(jax.random.fold_in(rng, 6), position), (parts,), jnp.float32, low / len(pieces), high / len(pieces))
        return jnp.repeat(jnp.exp(steps), shape[position] // parts).reshape((-1,) + (1,) * (len(shape) - position - 1))

    gain = one(*pieces[0])
    for cut in pieces[1:]:
        gain = gain * one(*cut)
    return gain


def bell_draw(rng, extent, deviation, limit, cuts=(), kind=jnp.bfloat16):
    loudness = block_scale(rng, extent, cuts, -0.22, 0.18) if cuts else 1.0
    values = jax.random.normal(rng, extent, jnp.float32) * deviation * loudness
    return jnp.minimum(jnp.maximum(values, -limit), limit).astype(kind)


def setup_inputs(seed: int = 0) -> dict:
    streams_of = jax.random.split(jax.random.key(seed), 7)
    residual = bell_draw(streams_of[0], (VARIABLES, AXIAL, SPANWISE_VOLUMES, NP), 0.1, 0.6, ((2, 8), (3, 4)), jnp.float32)
    inverse_diagonal = draw_inverse_diagonal(jax.random.fold_in(streams_of[6], 71), 0)
    prior_increment = bell_draw(streams_of[2], (VARIABLES, AXIAL, SPANWISE_VOLUMES, NP), 0.5, 3.0, ((2, 8), (3, 4)), jnp.float32)
    coupling = draw_coupling(jax.random.fold_in(streams_of[6], 71), 0)
    characteristic = bell_draw(streams_of[4], (2, 2, HARMONICS, VARIABLES, VARIABLES), 1.0, 6.0, (), jnp.float32)
    cutoffs = jax.random.randint(streams_of[5], (2,), HARMONICS // 4, HARMONICS + 1).astype(jnp.int32)
    return {"residual": residual, "inverse_diagonal": inverse_diagonal, "prior_increment": prior_increment, "coupling": coupling, "characteristic": characteristic, "cutoffs": cutoffs}


highest = lax.Precision.HIGHEST


def angle_tables(pitch_index, harmonic_index, points):
    product = (pitch_index[:, None] * harmonic_index[None, :]) % points
    angles = product.astype(jnp.float32) * (2.0 * jnp.pi / points)
    return jnp.cos(angles), jnp.sin(angles)


def forward_dft(spanwise_slices, cosine, sine):
    flat = spanwise_slices.reshape(-1, spanwise_slices.shape[-1])
    shape = spanwise_slices.shape[:-1] + (cosine.shape[1],)
    real_part = jnp.dot(flat, cosine, precision=highest).reshape(shape)
    imag_part = -jnp.dot(flat, sine, precision=highest).reshape(shape)
    return real_part, imag_part


def contract(matrix, spectrum):
    return jnp.einsum('pkij,pjrk->pirk', matrix, spectrum, precision=highest)


def apply_harmonics(real_part, imag_part, characteristic, cutoffs, first_harmonic, points):
    char_real = characteristic[:, 0]
    char_imag = characteristic[:, 1]
    result_real_component = contract(char_real, real_part) - contract(char_imag, imag_part)
    out_imag = contract(char_real, imag_part) + contract(char_imag, real_part)
    harmonic = first_harmonic + jnp.arange(real_part.shape[-1], dtype=jnp.int32)
    kept = (harmonic[None, :] < cutoffs[:, None]).astype(jnp.float32)
    weight = jnp.where(harmonic == 0, 1.0, 2.0).astype(jnp.float32) / points
    factor = (kept * weight[None, :])[:, None, None, :]
    return result_real_component * factor, out_imag * factor


def inverse_dft(result_real_component, out_imag, cosine, sine):
    shape = result_real_component.shape[:-1] + (cosine.shape[0],)
    flat_real = result_real_component.reshape(-1, result_real_component.shape[-1])
    flat_imag = out_imag.reshape(-1, out_imag.shape[-1])
    result = jnp.dot(flat_real, cosine.T, precision=highest) - jnp.dot(flat_imag, sine.T, precision=highest)
    return result.reshape(shape)


def mix_field(matrix, field):
    return jnp.einsum('ij,jarp->iarp', matrix, field, precision=highest)


def mix_vector(matrix, vector):
    return jnp.einsum('ij,jap->iap', matrix, vector, precision=highest)


def apply_block(block, vector):
    return jnp.einsum('ijap,jap->iap', block, vector, precision=highest)


def reference(residual, inverse_diagonal, prior_increment, coupling, characteristic, cutoffs):
    spanwise_slices = jnp.stack([residual[:, 0], residual[:, -1]])
    pitch_index = jnp.arange(NP, dtype=jnp.int32)
    harmonic_index = jnp.arange(HARMONICS, dtype=jnp.int32)
    cosine, sine = angle_tables(pitch_index, harmonic_index, NP)
    real_part, imag_part = forward_dft(spanwise_slices, cosine, sine)
    result_real_component, out_imag = apply_harmonics(real_part, imag_part, characteristic, cutoffs, 0, NP)
    correction = inverse_dft(result_real_component, out_imag, cosine, sine)
    corrected = residual.at[:, 0].add(correction[0]).at[:, -1].add(correction[1])
    padded = jnp.concatenate([prior_increment[..., -1:], prior_increment, prior_increment[..., :1]], axis=3)
    axial_pad = jnp.pad(prior_increment, ((0, 0), (1, 1), (0, 0), (0, 0)))
    source = corrected - mix_field(coupling[2], padded[..., :-2]) - mix_field(coupling[3], padded[..., 2:])
    source = source - mix_field(coupling[4], axial_pad[:, :-2]) - mix_field(coupling[5], axial_pad[:, 2:])
    diag_rows = jnp.moveaxis(inverse_diagonal, 3, 0)
    source_rows = jnp.moveaxis(source, 2, 0)
    zeros = jnp.zeros((residual.shape[0], residual.shape[1], residual.shape[3]), jnp.float32)

    def forward_sweep_step(previous, pair):
        block, rhs_row = pair
        current = apply_block(block, rhs_row - mix_vector(coupling[0], previous))
        return current, current

    _, star_rows = lax.scan(forward_sweep_step, zeros, (diag_rows, source_rows))

    def backward_step(following, pair):
        block, star_row = pair
        current = star_row - apply_block(block, mix_vector(coupling[1], following))
        return current, current

    _, final_rows = lax.scan(backward_step, zeros, (diag_rows, star_rows), reverse=True)
    return jnp.moveaxis(final_rows, 0, 2)
```

```python
import functools

import jax
import jax.numpy as jnp
import ml_dtypes
import numpy as np
from jax import lax
from jax.experimental import pallas as pl
from jax.experimental.pallas import tpu as pltpu
from jax.sharding import PartitionSpec as P

LANES = 128
HALF = 64
VMEM = pl.BlockSpec(memory_space=pltpu.VMEM)
SMEM = pl.BlockSpec(memory_space=pltpu.SMEM)
F32 = jnp.float32
BF16 = jnp.bfloat16


def call(kernel, outs, ins, specs, scratch=(), flops=1_000_000):
    moved = 4 * sum(int(np.prod(a.shape)) for a in ins)
    return pl.pallas_call(
        kernel,
        out_shape=[jax.ShapeDtypeStruct(s, F32) for s in outs],
        in_specs=list(specs),
        out_specs=[VMEM] * len(outs),
        scratch_shapes=list(scratch),
        cost_estimate=pl.CostEstimate(flops=flops, bytes_accessed=moved, transcendentals=0),
        compiler_params=pltpu.CompilerParams(vmem_limit_bytes=24 * 1024 * 1024),
    )(*ins)


def total(terms):
    result = terms[0]
    for term in terms[1:]:
        result = result + term
    return result


def matvec(get, vector):
    size = len(vector)
    return [total([get(i, j) * vector[j] for j in range(size)]) for i in range(size)]


def plus(a, b):
    return [x + y for x, y in zip(a, b)]


def split(x):
    high = x.astype(BF16)
    return high, (x - high.astype(F32)).astype(BF16)


class Sizes:
    def __init__(self, residual, characteristic, pitch):
        self.v, self.axial, self.rows, self.width = residual.shape
        self.tiles = self.width // LANES
        self.block = self.tiles * self.rows
        self.cells = self.axial * self.tiles
        self.n = pitch
        self.points = pitch * self.width
        self.harmonics = characteristic.shape[2]
        self.per = self.harmonics // pitch
        self.planes = 2 * self.v * self.block
        self.vv = self.v * self.v


def to_tiles(array, sizes):
    lead = array.shape[:-3]
    array = array.reshape(lead + (sizes.axial, sizes.rows, sizes.tiles, LANES))
    array = jnp.swapaxes(array, -3, -2)
    return array.reshape((-1, sizes.axial * sizes.block, LANES))


def from_tiles(array, sizes):
    array = array.reshape((sizes.v, sizes.axial, sizes.tiles, sizes.rows, LANES))
    array = jnp.swapaxes(array, -3, -2)
    return array.reshape((sizes.v, sizes.axial, sizes.rows, sizes.width))


def payload_kernel(z, residual, prior, out):
    for q, a in enumerate((0, z.axial - 1)):
        for v in range(z.v):
            out[pl.ds((q * z.v + v) * z.block, z.block), :] = residual[
                v, pl.ds(a * z.block, z.block), :
            ]
    lane = lax.broadcasted_iota(jnp.int32, (z.rows, LANES), 1)
    halo = jnp.zeros((z.rows, LANES), F32)
    for v in range(z.v):
        for a in range(z.axial):
            first = prior[v, pl.ds(a * z.block, z.rows), :][:, 0:1]
            last = prior[v, pl.ds((a + 1) * z.block - z.rows, z.rows), :][:, LANES - 1 :]
            halo = jnp.where(lane == v * z.axial + a, first, halo)
            halo = jnp.where(lane == HALF + v * z.axial + a, last, halo)
    out[pl.ds(z.planes, z.rows), :] = halo


def maps_kernel(
    z, diag, residual, prior, char, coupling, cutoffs, ops, maps, source, spec, blocks, powers
):
    span = range(z.v)
    vv = z.vv

    def scalar(which, i, j):
        return coupling[which * vv + i * z.v + j]

    def operators(r, _):
        for i in span:
            d = [diag[i * z.v + j, pl.ds(r, z.cells, stride=z.rows), :] for j in span]
            for k in span:
                ops[r, i * z.v + k] = -total([d[j] * scalar(0, j, k) for j in span])
                ops[r, vv + i * z.v + k] = -total([d[j] * scalar(1, j, k) for j in span])
                ops[r, 2 * vv + i * z.v + k] = d[k]
        return 0

    lax.fori_loop(0, z.rows, operators, 0)

    for m in range(vv):
        powers[0, m] = ops[0, m]

    def forward(r, _):
        for k in span:
            column = [powers[r - 1, j * z.v + k] for j in span]
            new = matvec(lambda i, j: ops[r, i * z.v + j], column)
            for i in span:
                powers[r, i * z.v + k] = new[i]
        return 0

    lax.fori_loop(1, z.rows, forward, 0)
    top = z.rows - 1
    for m in range(vv):
        maps[m] = powers[top, m]
        maps[vv + m] = powers[top, m]
        maps[2 * vv + m] = ops[top, vv + m]

    def backward(step, _):
        r = top - step
        for k in span:
            for base in (vv, 2 * vv):
                column = [maps[base + j * z.v + k] for j in span]
                new = matvec(lambda i, j: ops[r, vv + i * z.v + j], column)
                for i in span:
                    value = new[i]
                    if base == vv:
                        value = value + powers[r, i * z.v + k]
                    maps[base + i * z.v + k] = value
        return 0

    lax.fori_loop(1, z.rows, backward, 0)

    lane = lax.broadcasted_iota(jnp.int32, (z.rows, LANES), 1)

    def tile(ref, v, a, h):
        return ref[v, pl.ds(a * z.block + h * z.rows, z.rows), :]

    for a in range(z.axial):
        here = [[tile(prior, v, a, h) for h in range(z.tiles)] for v in span]
        up = [[pltpu.roll(x, 1, 1) for x in row] for row in here]
        down = [[pltpu.roll(x, LANES - 1, 1) for x in row] for row in here]
        for h in range(z.tiles):
            lower, upper = [], []
            for v in span:
                edge = up[v][h - 1] if h else jnp.zeros((z.rows, LANES), F32)
                lower.append(jnp.where(lane == 0, edge, up[v][h]))
                edge = down[v][h + 1] if h + 1 < z.tiles else jnp.zeros((z.rows, LANES), F32)
                upper.append(jnp.where(lane == LANES - 1, edge, down[v][h]))
            terms = [(2, lower), (3, upper)]
            if a > 0:
                terms.append((4, [tile(prior, v, a - 1, h) for v in span]))
            if a + 1 < z.axial:
                terms.append((5, [tile(prior, v, a + 1, h) for v in span]))
            for i in span:
                value = tile(residual, i, a, h)
                for which, field in terms:
                    value = value - total([field[j] * scalar(which, i, j) for j in span])
                source[i, pl.ds(a * z.block + h * z.rows, z.rows), :] = value

    k_of = lax.broadcasted_iota(jnp.int32, (z.harmonics, z.harmonics), 0)
    place = lax.broadcasted_iota(jnp.int32, (z.harmonics, z.harmonics), 1)
    wanted = (place % z.per) * z.n + place // z.per
    select = jnp.where(k_of == wanted, 1.0, 0.0).astype(BF16)
    value = char[...]
    high, rest = split(value)
    rest = value - high.astype(F32)
    middle, low = split(rest)
    ordered = total(
        [jnp.dot(part, select, preferred_element_type=F32) for part in (high, middle, low)]
    )
    row = lax.broadcasted_iota(jnp.int32, ordered.shape, 0)
    place = lax.broadcasted_iota(jnp.int32, ordered.shape, 1)
    harmonic = (place % z.per) * z.n + place // z.per
    cutoff = jnp.where(row < ordered.shape[0] // 2, cutoffs[0], cutoffs[1])
    weight = jnp.where(harmonic == 0, 1.0, 2.0) / z.points
    spec[...] = ordered * jnp.where(harmonic < cutoff, weight, 0.0)


def spectral_kernel(z, *refs):
    blocks = refs[: z.n]
    table_high, table_low, spec, ops, source, coupling, driven, vectors, real, imag, total_source = (
        refs[z.n :]
    )
    span = range(z.v)
    vv = z.vv
    flat = 2 * z.v * z.rows

    def scalar(which, i, j):
        return coupling[which * vv + i * z.v + j]

    def plane(ref):
        value = ref[pl.ds(0, z.planes), :].reshape(2 * z.v, z.tiles, z.rows, LANES)
        parts = [value[:, h].reshape(flat, LANES) for h in range(z.tiles)]
        return parts[0] if len(parts) == 1 else jnp.concatenate(parts, axis=1)

    x = [plane(ref) for ref in blocks]

    def combine(coefficients):
        terms = []
        for c, value in zip(coefficients, x):
            if abs(c) < 1e-12:
                continue
            if abs(c - 1) < 1e-12:
                terms.append(value)
            elif abs(c + 1) < 1e-12:
                terms.append(-value)
            else:
                terms.append(value * float(c))
        return total(terms) if terms else None

    def table(ref, s):
        return ref[:, pl.ds(2 * z.per * s, 2 * z.per)]

    turns = 2 * np.pi * np.arange(z.n) / z.n
    for s in range(z.n // 2 + 1):
        yr = combine(np.cos(turns * s))
        yi = combine(-np.sin(turns * s))
        highs, lows = zip(*[split(y) for y in (yr, yi) if y is not None])
        both = jnp.concatenate(highs + lows, axis=0)
        high = jnp.concatenate(highs, axis=0) if len(highs) > 1 else highs[0]
        rows = high.shape[0]
        for t in sorted({s, (z.n - s) % z.n}):
            first = jnp.dot(both, table(table_high, t), preferred_element_type=F32)
            second = jnp.dot(high, table(table_low, t), preferred_element_type=F32)
            y = first[:rows] + first[rows:] + second
            re, im = y[:flat, : z.per], -y[:flat, z.per :]
            if yi is not None:
                sign = 1.0 if t == s else -1.0
                re = re + sign * y[flat:, z.per :]
                im = im + sign * y[flat:, : z.per]
            real[:, pl.ds(z.per * t, z.per)] = re
            imag[:, pl.ds(z.per * t, z.per)] = im

    out_real, out_imag = [], []
    for q in range(2):
        rows = [pl.ds((q * z.v + j) * z.rows, z.rows) for j in span]
        re = [real[at, :] for at in rows]
        im = [imag[at, :] for at in rows]
        for i in span:
            base = 2 * ((q * z.v + i) * z.v)
            cr = [spec[pl.ds(base + 2 * j, 1), :] for j in span]
            ci = [spec[pl.ds(base + 2 * j + 1, 1), :] for j in span]
            out_real.append(total([cr[j] * re[j] - ci[j] * im[j] for j in span]))
            out_imag.append(total([cr[j] * im[j] + ci[j] * re[j] for j in span]))
    cr = jnp.concatenate(out_real, axis=0)
    ci = -jnp.concatenate(out_imag, axis=0)
    parts = []
    for s in range(z.n):
        at = slice(s * z.per, (s + 1) * z.per)
        parts += [cr[:, at], ci[:, at]]
    high, low = split(jnp.concatenate(parts, axis=1))
    dims = (((1,), (1,)), ((), ()))
    both = jnp.concatenate([high, low], axis=0)
    first = lax.dot_general(both, table_high[...], dims, preferred_element_type=F32)
    second = lax.dot_general(high, table_low[...], dims, preferred_element_type=F32)
    correction = first[:flat] + first[flat:] + second

    lane = lax.broadcasted_iota(jnp.int32, (z.rows, LANES), 1)
    before = blocks[z.n - 1][pl.ds(z.planes, z.rows), :]
    after = blocks[1][pl.ds(z.planes, z.rows), :]
    for a in range(z.axial):
        lows = [before[:, HALF + v * z.axial + a : HALF + v * z.axial + a + 1] for v in span]
        highs = [after[:, v * z.axial + a : v * z.axial + a + 1] for v in span]
        for h in range(z.tiles):
            at = pl.ds(a * z.block + h * z.rows, z.rows)
            for i in span:
                value = source[i, at, :]
                if h == 0:
                    edge = total([lows[j] * scalar(2, i, j) for j in span])
                    value = value - jnp.where(lane == 0, edge, 0.0)
                if h == z.tiles - 1:
                    edge = total([highs[j] * scalar(3, i, j) for j in span])
                    value = value - jnp.where(lane == LANES - 1, edge, 0.0)
                for q, plane_a in enumerate((0, z.axial - 1)):
                    if a == plane_a:
                        first = (q * z.v + i) * z.rows
                        value = value + correction[
                            first : first + z.rows, h * LANES : (h + 1) * LANES
                        ]
                total_source[i, at, :] = value

    def drive(r, _):
        row = [total_source[j, pl.ds(r, z.cells, stride=z.rows), :] for j in span]
        new = matvec(lambda i, j: ops[r, 2 * vv + i * z.v + j], row)
        for i in span:
            driven[r, i] = new[i]
        return 0

    lax.fori_loop(0, z.rows, drive, 0)
    stars = [[driven[0, i] for i in span]]
    for r in range(1, z.rows):
        moved = matvec(lambda i, j: ops[r, i * z.v + j], stars[-1])
        stars.append([driven[r, i] + moved[i] for i in span])
    back = stars[-1]
    for r in range(z.rows - 2, -1, -1):
        back = plus(stars[r], matvec(lambda i, j: ops[r, vv + i * z.v + j], back))
    for i in span:
        vectors[i] = stars[-1][i]
        vectors[z.v + i] = back[i]


def merge_maps_kernel(size, radix, where, *refs):
    members, out, slots = refs[:radix], refs[radix], refs[radix + 1]
    vv = size * size
    place_members(radix, where, members, slots)
    span = range(size)

    def column(w, base, k):
        return [slots[w, base + j * size + k] for j in span]

    def apply(w, base, vector):
        return matvec(lambda i, j: slots[w, base + i * size + j], vector)

    for k in span:
        states = [None, column(0, 0, k)]
        for w in range(1, radix):
            states.append(apply(w, 0, states[-1]))
        back = None
        through = None
        for w in range(radix - 1, -1, -1):
            mine = column(0, vv, k) if w == 0 else apply(w, vv, states[w])
            back = mine if back is None else plus(mine, apply(w, 2 * vv, back))
            through = column(w, 2 * vv, k) if through is None else apply(w, 2 * vv, through)
        for i in span:
            out[i * size + k] = states[-1][i]
            out[vv + i * size + k] = back[i]
            out[2 * vv + i * size + k] = through[i]


def place_members(radix, where, members, slots):
    own = where[0]
    for t, ref in enumerate(members):
        slots[lax.rem(own + t, radix)] = ref[...]


def merge_vectors_kernel(size, radix, where, *refs):
    maps, vectors = refs[:radix], refs[radix : 2 * radix]
    out, map_slots, vector_slots = refs[2 * radix :]
    place_members(radix, where, maps, map_slots)
    place_members(radix, where, vectors, vector_slots)
    vv = size * size
    span = range(size)

    def apply(w, base, vector):
        return matvec(lambda i, j: map_slots[w, base + i * size + j], vector)

    def given(w, base):
        return [vector_slots[w, base + i] for i in span]

    states = [None, given(0, 0)]
    for w in range(1, radix):
        states.append(plus(apply(w, 0, states[-1]), given(w, 0)))
    back = None
    for w in range(radix - 1, -1, -1):
        mine = given(w, size)
        if w:
            mine = plus(mine, apply(w, vv, states[w]))
        back = mine if back is None else plus(mine, apply(w, 2 * vv, back))
    for i in span:
        out[i] = states[-1][i]
        out[size + i] = back[i]


def final_kernel(z, radices, where, *refs):
    span = range(z.v)
    vv = z.vv
    refs = list(refs)
    levels = []
    for radix in radices:
        levels.append((refs[:radix], refs[radix : 2 * radix]))
        refs = refs[2 * radix :]
    ops, driven, out, pairs, stars = refs[:5]
    scratch = refs[5:]
    x = y = None
    for level in range(len(radices) - 1, -1, -1):
        radix = radices[level]
        maps, vectors = levels[level]
        map_slots, vector_slots = scratch[2 * level : 2 * level + 2]
        own = where[level]
        for t in range(radix):
            at = lax.rem(own + t, radix)
            map_slots[at] = maps[t][...]
            vector_slots[at] = vectors[t][...]

        def apply(w, base, vector):
            return matvec(lambda i, j: map_slots[w, base + i * z.v + j], vector)

        def given(w, base):
            return [vector_slots[w, base + i] for i in span]

        states = [x]
        for w in range(radix - 1):
            new = given(w, 0)
            states.append(new if states[-1] is None else plus(new, apply(w, 0, states[-1])))
        for w in range(radix):
            for i in span:
                pairs[w, i] = jnp.zeros_like(pairs[w, i]) if states[w] is None else states[w][i]
        back = y
        for w in range(radix - 1, -1, -1):
            for i in span:
                pairs[w, z.v + i] = jnp.zeros_like(pairs[w, i]) if back is None else back[i]
            if w:
                mine = plus(given(w, z.v), apply(w, vv, states[w]))
                back = mine if back is None else plus(mine, apply(w, 2 * vv, back))
        x = [pairs[own, i] for i in span]
        y = [pairs[own, z.v + i] for i in span]

    for r in range(z.rows):
        x = plus([driven[r, i] for i in span], matvec(lambda i, j: ops[r, i * z.v + j], x))
        for i in span:
            stars[r, i] = x[i]
    for r in range(z.rows - 1, -1, -1):
        y = plus(
            [stars[r, i] for i in span], matvec(lambda i, j: ops[r, vv + i * z.v + j], y)
        )
        for i in span:
            out[i, pl.ds(r, z.cells, stride=z.rows), :] = y[i]


def trig_tables(z):
    q = np.arange(z.width)[:, None]
    k = (np.arange(z.n)[:, None] + z.n * np.arange(z.per)[None, :]).reshape(1, z.n, 1, z.per)
    angle = 2 * np.pi * ((q.reshape(-1, 1, 1, 1) * k) % z.points) / z.points
    values = np.concatenate([np.cos(angle), np.sin(angle)], axis=2).reshape(z.width, -1)
    high = values.astype(np.float32).astype(ml_dtypes.bfloat16)
    low = (values - high.astype(np.float64)).astype(np.float32).astype(ml_dtypes.bfloat16)
    return high, low


def radices_of(count):
    found = []
    while count > 1:
        radix = 4 if count % 4 == 0 and (found or count == 4) else 2 if count % 2 == 0 else count
        found.append(radix)
        count //= radix
    return found


def body(residual, inverse_diagonal, prior_increment, coupling, characteristic, cutoffs):
    pitch, span = lax.axis_size("pitch"), lax.axis_size("span")
    z = Sizes(residual, characteristic, pitch)
    vv = z.vv
    residual_t = to_tiles(residual, z)
    prior_t = to_tiles(prior_increment, z)
    diag_t = to_tiles(inverse_diagonal, z)
    couple = coupling.reshape(-1)
    char = jnp.transpose(characteristic, (0, 3, 4, 1, 2)).reshape(-1, z.harmonics)

    payload = call(
        functools.partial(payload_kernel, z),
        [(z.planes + z.rows, LANES)],
        (residual_t, prior_t),
        [VMEM] * 2,
    )[0]
    blocks = [payload]
    for j in range(1, pitch):
        blocks.append(lax.ppermute(payload, "pitch", [((e + j) % pitch, e) for e in range(pitch)]))

    cell = (z.cells, LANES)
    ops, maps, source, spec = call(
        functools.partial(maps_kernel, z),
        [
            (z.rows, 3 * vv) + cell,
            (3 * vv,) + cell,
            (z.v, z.axial * z.block, LANES),
            char.shape,
        ],
        (diag_t, residual_t, prior_t, char, couple, cutoffs),
        [VMEM] * 4 + [SMEM] * 2,
        [pltpu.VMEM((8, LANES), F32), pltpu.VMEM((z.rows, vv) + cell, F32)],
        flops=20_000_000,
    )

    device = lax.axis_index("span")
    radices = radices_of(span)
    where, map_levels, stride = [], [], 1
    strides = []
    for level, radix in enumerate(radices):
        own = (device // stride) % radix
        where.append(own.astype(jnp.int32).reshape(1))
        strides.append(stride)
        others = gather(maps, span, stride, radix)
        map_levels.append([maps] + others)
        if level + 1 < len(radices):
            maps = call(
                functools.partial(merge_maps_kernel, z.v, radix),
                [(3 * vv,) + cell],
                (where[-1], *map_levels[-1]),
                [SMEM] + [VMEM] * radix,
                [pltpu.VMEM((radix, 3 * vv) + cell, F32)],
                flops=5_000_000,
            )[0]
        stride *= radix

    high, low = trig_tables(z)
    driven, vectors = call(
        functools.partial(spectral_kernel, z),
        [(z.rows, z.v) + cell, (2 * z.v,) + cell],
        (*blocks, jnp.asarray(high), jnp.asarray(low), spec, ops, source, couple),
        [VMEM] * (z.n + 5) + [SMEM],
        [
            pltpu.VMEM((2 * z.v * z.rows, z.harmonics), F32),
            pltpu.VMEM((2 * z.v * z.rows, z.harmonics), F32),
            pltpu.VMEM((z.v, z.axial * z.block, LANES), F32),
        ],
        flops=20_000_000,
    )

    vector_levels = []
    for level, radix in enumerate(radices):
        others = gather(vectors, span, strides[level], radix)
        vector_levels.append([vectors] + others)
        if level + 1 < len(radices):
            vectors = call(
                functools.partial(merge_vectors_kernel, z.v, radix),
                [(2 * z.v,) + cell],
                (where[level], *map_levels[level], *vector_levels[level]),
                [SMEM] + [VMEM] * (2 * radix),
                [
                    pltpu.VMEM((radix, 3 * vv) + cell, F32),
                    pltpu.VMEM((radix, 2 * z.v) + cell, F32),
                ],
            )[0]

    arrays, scratch = [], []
    for level, radix in enumerate(radices):
        arrays += map_levels[level] + vector_levels[level]
        scratch += [
            pltpu.VMEM((radix, 3 * vv) + cell, F32),
            pltpu.VMEM((radix, 2 * z.v) + cell, F32),
        ]
    update = call(
        functools.partial(final_kernel, z, radices),
        [(z.v, z.axial * z.block, LANES)],
        (jnp.concatenate(where), *arrays, ops, driven),
        [SMEM] + [VMEM] * (len(arrays) + 2),
        [
            pltpu.VMEM((max(radices), 2 * z.v) + cell, F32),
            pltpu.VMEM((z.rows, z.v) + cell, F32),
            *scratch,
        ],
        flops=2_000_000,
    )[0]
    return from_tiles(update, z)


def gather(value, span, stride, radix):
    others = []
    for t in range(1, radix):
        pairs = []
        for d in range(span):
            g = (d // stride) % radix
            pairs.append((d + ((g + t) % radix - g) * stride, d))
        others.append(lax.ppermute(value, "span", pairs))
    return others


def solution(mesh):
    in_specs = (
        P(None, None, "span", "pitch"),
        P(None, None, None, "span", "pitch"),
        P(None, None, "span", "pitch"),
        P(),
        P(),
        P(),
    )
    out_specs = P(None, None, "span", "pitch")
    return jax.shard_map(body, mesh=mesh, in_specs=in_specs, out_specs=out_specs, check_vma=False)
```

```python
import functools

import jax
import jax.numpy as jnp
import ml_dtypes
import numpy as np
from jax import lax
from jax.experimental import pallas as pl
from jax.experimental.pallas import tpu as pltpu
from jax.sharding import PartitionSpec as P


LANES = 128
HALF = 64
VMEM = pl.BlockSpec(memory_space=pltpu.VMEM)
SMEM = pl.BlockSpec(memory_space=pltpu.SMEM)
HBM = pl.BlockSpec(memory_space=pltpu.HBM)
ANY = pl.BlockSpec(memory_space=pl.ANY)
PARTS = 1
F32 = jnp.float32
BF16 = jnp.bfloat16


def call(kernel, outs, ins, specs, scratch=(), flops=1_000_000):
    moved = 4 * sum(int(np.prod(a.shape)) for a in ins)
    ins = [
        pltpu.with_memory_space_constraint(a, pltpu.HBM) if spec is HBM else a
        for a, spec in zip(ins, specs)
    ]
    return kernel_call(kernel, outs, ins, specs, scratch, flops, moved)


def kernel_call(kernel, outs, ins, specs, scratch, flops, moved):
    return pl.pallas_call(
        kernel,
        out_shape=[
            jax.ShapeDtypeStruct(*s) if isinstance(s[0], tuple) else jax.ShapeDtypeStruct(s, F32)
            for s in outs
        ],
        in_specs=list(specs),
        out_specs=[VMEM] * len(outs),
        scratch_shapes=list(scratch),
        cost_estimate=pl.CostEstimate(flops=flops, bytes_accessed=moved, transcendentals=0),
        compiler_params=pltpu.CompilerParams(vmem_limit_bytes=12 * 1024 * 1024),
    )(*ins)


def total(terms):
    result = terms[0]
    for term in terms[1:]:
        result = result + term
    return result


def matvec(get, vector):
    size = len(vector)
    return [total([get(i, j) * vector[j] for j in range(size)]) for i in range(size)]


def plus(a, b):
    return [x + y for x, y in zip(a, b)]


def split(x):
    high = x.astype(BF16)
    return high, (x - high.astype(F32)).astype(BF16)


def splat(coupling, which, i, j, shape):
    return jnp.broadcast_to(coupling[i, which : which + 1, j : j + 1], shape)


class Sizes:
    def __init__(self, residual, characteristic, pitch):
        self.v, self.axial, self.rows, self.width = residual.shape
        self.tiles = self.width // LANES
        self.block = self.tiles * self.rows
        self.cells = self.axial * self.tiles
        self.n = pitch
        self.points = pitch * self.width
        self.harmonics = characteristic.shape[2]
        self.per = self.harmonics // pitch
        self.planes = 2 * self.v * self.block
        self.vv = self.v * self.v
        self.parts = PARTS
        self.chunk = self.cells // self.parts


def to_tiles(array, sizes):
    lead = array.shape[:-3]
    array = array.reshape(lead + (sizes.axial, sizes.rows, sizes.tiles, LANES))
    array = jnp.swapaxes(array, -3, -2)
    return array.reshape((-1, sizes.axial * sizes.block, LANES))


def from_tiles(array, sizes):
    array = array.reshape((sizes.v, sizes.axial, sizes.tiles, sizes.rows, LANES))
    array = jnp.swapaxes(array, -3, -2)
    return array.reshape((sizes.v, sizes.axial, sizes.rows, sizes.width))


def payload_kernel(z, residual, prior, out, edges, sems):
    copies = []
    for q, a in enumerate((0, z.axial - 1)):
        for v in range(z.v):
            m = q * z.v + v
            copies.append(
                pltpu.make_async_copy(
                    residual.at[v, pl.ds(a * z.block, z.block), :],
                    out.at[pl.ds(m * z.block, z.block), :],
                    sems.at[m],
                )
            )
    copies.append(pltpu.make_async_copy(prior, edges, sems.at[2 * z.v]))
    for copy in copies[::-1]:
        copy.start()
    copies[-1].wait()
    lane = lax.broadcasted_iota(jnp.int32, (z.rows, LANES), 1)
    halo = jnp.zeros((z.rows, LANES), F32)
    for v in range(z.v):
        for a in range(z.axial):
            first = edges[v, pl.ds(a * z.block, z.rows), :][:, 0:1]
            last = edges[v, pl.ds((a + 1) * z.block - z.rows, z.rows), :][:, LANES - 1 :]
            halo = jnp.where(lane == v * z.axial + a, first, halo)
            halo = jnp.where(lane == HALF + v * z.axial + a, last, halo)
    out[pl.ds(z.planes, z.rows), :] = halo
    for copy in copies[:-1]:
        copy.wait()


def maps_kernel(z, diag_h, coupling_h, after, ops, *refs):
    del after
    outs, (maps, powers, diag, coupling, splats, sems) = refs[: z.parts], refs[z.parts :]
    span = range(z.v)
    vv = z.vv
    copies = [
        pltpu.make_async_copy(coupling_h, coupling, sems.at[0]),
        pltpu.make_async_copy(diag_h, diag, sems.at[1]),
    ]
    for copy in copies:
        copy.start()
    copies[0].wait()
    for which in range(2):
        for i in span:
            for j in span:
                splats[which * vv + i * z.v + j] = splat(
                    coupling, which, i, j, (z.cells, LANES)
                )
    copies[1].wait()

    def operators(r, _):
        for i in span:
            d = [diag[i * z.v + j, pl.ds(r, z.cells, stride=z.rows), :] for j in span]
            for k in span:
                for which in range(2):
                    ops[r, which * vv + i * z.v + k] = -total(
                        [d[j] * splats[which * vv + j * z.v + k] for j in span]
                    )
                ops[r, 2 * vv + i * z.v + k] = d[k]
        return 0

    lax.fori_loop(0, z.rows, operators, 0)

    for m in range(vv):
        powers[0, m] = ops[0, m]

    def forward(r, _):
        for k in span:
            column = [powers[r - 1, j * z.v + k] for j in span]
            new = matvec(lambda i, j: ops[r, i * z.v + j], column)
            for i in span:
                powers[r, i * z.v + k] = new[i]
        return 0

    lax.fori_loop(1, z.rows, forward, 0)
    top = z.rows - 1
    for m in range(vv):
        maps[m] = powers[top, m]
        maps[vv + m] = powers[top, m]
        maps[2 * vv + m] = ops[top, vv + m]

    def backward(step, _):
        r = top - step
        for k in span:
            for base in (vv, 2 * vv):
                column = [maps[base + j * z.v + k] for j in span]
                new = matvec(lambda i, j: ops[r, vv + i * z.v + j], column)
                for i in span:
                    value = new[i]
                    if base == vv:
                        value = value + powers[r, i * z.v + k]
                    maps[base + i * z.v + k] = value
        return 0

    lax.fori_loop(1, z.rows, backward, 0)
    for part in range(z.parts):
        for m in range(3 * vv):
            outs[part][m] = maps[m, pl.ds(part * z.chunk, z.chunk), :]


def prepare_kernel(z, *refs):
    residual_h, prior_h, char_h, high_h, low_h, coupling_h, cutoffs_h, after = refs[:8]
    source, spec, table_high, table_low, coupling, residual, prior, char, cutoffs, sems = refs[8:]
    del after
    span = range(z.v)
    vv = z.vv
    pairs = [
        (prior_h, prior),
        (residual_h, residual),
        (char_h, char),
        (high_h, table_high),
        (low_h, table_low),
        (coupling_h, coupling),
        (cutoffs_h, cutoffs),
    ]
    copies = [pltpu.make_async_copy(a, b, sems.at[k]) for k, (a, b) in enumerate(pairs)]
    for copy in copies:
        copy.start()

    for k in (5, 6, 0, 1):
        copies[k].wait()
    shape = (z.rows, LANES)
    factors = {
        (which, i, j): splat(coupling, which, i, j, shape)
        for which in range(2, 6)
        for i in span
        for j in span
    }

    def scalar(which, i, j):
        return factors[which, i, j]

    lane = lax.broadcasted_iota(jnp.int32, (z.rows, LANES), 1)

    def tile(ref, v, a, h):
        return ref[v, pl.ds(a * z.block + h * z.rows, z.rows), :]

    for a in range(z.axial):
        here = [[tile(prior, v, a, h) for h in range(z.tiles)] for v in span]
        up = [[pltpu.roll(x, 1, 1) for x in row] for row in here]
        down = [[pltpu.roll(x, LANES - 1, 1) for x in row] for row in here]
        for h in range(z.tiles):
            lower, upper = [], []
            for v in span:
                edge = up[v][h - 1] if h else jnp.zeros((z.rows, LANES), F32)
                lower.append(jnp.where(lane == 0, edge, up[v][h]))
                edge = down[v][h + 1] if h + 1 < z.tiles else jnp.zeros((z.rows, LANES), F32)
                upper.append(jnp.where(lane == LANES - 1, edge, down[v][h]))
            terms = [(2, lower), (3, upper)]
            if a > 0:
                terms.append((4, [tile(prior, v, a - 1, h) for v in span]))
            if a + 1 < z.axial:
                terms.append((5, [tile(prior, v, a + 1, h) for v in span]))
            for i in span:
                value = tile(residual, i, a, h)
                for which, field in terms:
                    value = value - total([field[j] * scalar(which, i, j) for j in span])
                source[i, pl.ds(a * z.block + h * z.rows, z.rows), :] = value

    k_of = lax.broadcasted_iota(jnp.int32, (z.harmonics, z.harmonics), 0)
    place = lax.broadcasted_iota(jnp.int32, (z.harmonics, z.harmonics), 1)
    wanted = (place % z.per) * z.n + place // z.per
    select = jnp.where(k_of == wanted, 1.0, 0.0).astype(BF16)
    copies[2].wait()
    for c in range(2):
        value = char[:, c, :]
        high, rest = split(value)
        rest = value - high.astype(F32)
        middle, low = split(rest)
        ordered = total(
            [jnp.dot(part, select, preferred_element_type=F32) for part in (high, middle, low)]
        )
        row = lax.broadcasted_iota(jnp.int32, ordered.shape, 0)
        place = lax.broadcasted_iota(jnp.int32, ordered.shape, 1)
        harmonic = (place % z.per) * z.n + place // z.per
        cutoff = jnp.where(row < vv, cutoffs[0], cutoffs[1])
        weight = jnp.where(harmonic == 0, 1.0, 2.0) / z.points
        spec[c] = ordered * jnp.where(harmonic < cutoff, weight, 0.0)
    copies[3].wait()
    copies[4].wait()


def spectral_kernel(z, *refs):
    blocks = refs[: z.n]
    table_high, table_low, spec, ops, source, coupling, driven, vectors, real, imag, total_source = (
        refs[z.n :]
    )
    span = range(z.v)
    vv = z.vv
    flat = 2 * z.v * z.rows

    def scalar(which, i, j):
        return coupling[i, which : which + 1, j : j + 1]

    def plane(ref):
        value = ref[pl.ds(0, z.planes), :].reshape(2 * z.v, z.tiles, z.rows, LANES)
        parts = [value[:, h].reshape(flat, LANES) for h in range(z.tiles)]
        return parts[0] if len(parts) == 1 else jnp.concatenate(parts, axis=1)

    x = [plane(ref) for ref in blocks]

    def combine(coefficients):
        terms = []
        for c, value in zip(coefficients, x):
            if abs(c) < 1e-12:
                continue
            if abs(c - 1) < 1e-12:
                terms.append(value)
            elif abs(c + 1) < 1e-12:
                terms.append(-value)
            else:
                terms.append(value * float(c))
        return total(terms) if terms else None

    def table(ref, s):
        return ref[:, pl.ds(2 * z.per * s, 2 * z.per)]

    turns = 2 * np.pi * np.arange(z.n) / z.n
    for s in range(z.n // 2 + 1):
        yr = combine(np.cos(turns * s))
        yi = combine(-np.sin(turns * s))
        highs, lows = zip(*[split(y) for y in (yr, yi) if y is not None])
        both = jnp.concatenate(highs + lows, axis=0)
        high = jnp.concatenate(highs, axis=0) if len(highs) > 1 else highs[0]
        rows = high.shape[0]
        for t in sorted({s, (z.n - s) % z.n}):
            first = jnp.dot(both, table(table_high, t), preferred_element_type=F32)
            second = jnp.dot(high, table(table_low, t), preferred_element_type=F32)
            y = first[:rows] + first[rows:] + second
            re, im = y[:flat, : z.per], -y[:flat, z.per :]
            if yi is not None:
                sign = 1.0 if t == s else -1.0
                re = re + sign * y[flat:, z.per :]
                im = im + sign * y[flat:, : z.per]
            real[:, pl.ds(z.per * t, z.per)] = re
            imag[:, pl.ds(z.per * t, z.per)] = im

    out_real, out_imag = [], []
    for q in range(2):
        rows = [pl.ds((q * z.v + j) * z.rows, z.rows) for j in span]
        re = [real[at, :] for at in rows]
        im = [imag[at, :] for at in rows]
        for i in span:
            base = (q * z.v + i) * z.v
            cr = [spec[0, pl.ds(base + j, 1), :] for j in span]
            ci = [spec[1, pl.ds(base + j, 1), :] for j in span]
            out_real.append(total([cr[j] * re[j] - ci[j] * im[j] for j in span]))
            out_imag.append(total([cr[j] * im[j] + ci[j] * re[j] for j in span]))
    cr = jnp.concatenate(out_real, axis=0)
    ci = -jnp.concatenate(out_imag, axis=0)
    parts = []
    for s in range(z.n):
        at = slice(s * z.per, (s + 1) * z.per)
        parts += [cr[:, at], ci[:, at]]
    high, low = split(jnp.concatenate(parts, axis=1))
    dims = (((1,), (1,)), ((), ()))
    both = jnp.concatenate([high, low], axis=0)
    first = lax.dot_general(both, table_high[...], dims, preferred_element_type=F32)
    second = lax.dot_general(high, table_low[...], dims, preferred_element_type=F32)
    correction = first[:flat] + first[flat:] + second

    lane = lax.broadcasted_iota(jnp.int32, (z.rows, LANES), 1)
    before = blocks[z.n - 1][pl.ds(z.planes, z.rows), :]
    after = blocks[1][pl.ds(z.planes, z.rows), :]
    for a in range(z.axial):
        lows = [before[:, HALF + v * z.axial + a : HALF + v * z.axial + a + 1] for v in span]
        highs = [after[:, v * z.axial + a : v * z.axial + a + 1] for v in span]
        for h in range(z.tiles):
            at = pl.ds(a * z.block + h * z.rows, z.rows)
            for i in span:
                value = source[i, at, :]
                if h == 0:
                    edge = total([lows[j] * scalar(2, i, j) for j in span])
                    value = value - jnp.where(lane == 0, edge, 0.0)
                if h == z.tiles - 1:
                    edge = total([highs[j] * scalar(3, i, j) for j in span])
                    value = value - jnp.where(lane == LANES - 1, edge, 0.0)
                for q, plane_a in enumerate((0, z.axial - 1)):
                    if a == plane_a:
                        first = (q * z.v + i) * z.rows
                        value = value + correction[
                            first : first + z.rows, h * LANES : (h + 1) * LANES
                        ]
                total_source[i, at, :] = value

    def drive(r, _):
        row = [total_source[j, pl.ds(r, z.cells, stride=z.rows), :] for j in span]
        new = matvec(lambda i, j: ops[r, 2 * vv + i * z.v + j], row)
        for i in span:
            driven[r, i] = new[i]
        return 0

    lax.fori_loop(0, z.rows, drive, 0)
    stars = [[driven[0, i] for i in span]]
    for r in range(1, z.rows):
        moved = matvec(lambda i, j: ops[r, i * z.v + j], stars[-1])
        stars.append([driven[r, i] + moved[i] for i in span])
    back = stars[-1]
    for r in range(z.rows - 2, -1, -1):
        back = plus(stars[r], matvec(lambda i, j: ops[r, vv + i * z.v + j], back))
    for i in span:
        vectors[i] = stars[-1][i]
        vectors[z.v + i] = back[i]


def place_pair(where, own, other, slots, lower, upper):
    def fill(a, b):
        for k, m in enumerate(lower):
            slots[k] = a[m]
        for k, m in enumerate(upper):
            slots[len(lower) + k] = b[m]

    @pl.when(where == 0)
    def _():
        fill(own, other)

    @pl.when(where != 0)
    def _():
        fill(other, own)


def merge_maps_kernel(z, level, last, device, own, other, out, slots):
    vv = z.vv
    every = list(range(3 * vv))
    place_pair((device[0] >> level) & 1, own, other, slots, every, every)
    span = range(z.v)

    def column(base, k):
        return [slots[base + j * z.v + k] for j in span]

    def apply(base, vector):
        return matvec(lambda i, j: slots[base + i * z.v + j], vector)

    up = 3 * vv
    for k in span:
        state = column(0, k)
        back = plus(column(vv, k), apply(2 * vv, apply(up + vv, state)))
        if last:
            for i in span:
                out[i * z.v + k] = back[i]
            continue
        state = apply(up, state)
        through = apply(2 * vv, column(up + 2 * vv, k))
        for i in span:
            out[i * z.v + k] = state[i]
            out[vv + i * z.v + k] = back[i]
            out[2 * vv + i * z.v + k] = through[i]


def merge_vectors_kernel(z, level, device, *refs):
    own_maps, other_maps = refs[: z.parts], refs[z.parts : 2 * z.parts]
    own, other, out, slots, vectors = refs[2 * z.parts :]
    vv = z.vv
    span = range(z.v)
    bit = (device[0] >> level) & 1
    every = list(range(2 * z.v))
    place_pair(bit, own, other, vectors, every, every)
    for part in range(z.parts):
        at = pl.ds(part * z.chunk, z.chunk)
        place_pair(
            bit, own_maps[part], other_maps[part], slots, range(2 * vv, 3 * vv), range(2 * vv)
        )

        def apply(base, vector):
            return matvec(lambda i, j: slots[base + i * z.v + j], vector)

        fa, ha, fb, hb = [[vectors[k * z.v + i, at, :] for i in span] for k in range(4)]
        state = plus(fb, apply(vv, fa))
        back = plus(ha, apply(0, plus(hb, apply(2 * vv, fa))))
        for i in span:
            out[i, at, :] = state[i]
            out[z.v + i, at, :] = back[i]


def final_kernel(z, levels, device, *refs):
    span = range(z.v)
    vv = z.vv
    refs = list(refs)

    def take(count):
        taken = refs[:count]
        del refs[:count]
        return taken

    inner_maps = [(take(z.parts), take(z.parts)) for _ in range(levels - 1)]
    outer = take(z.parts)
    vector_pairs = [take(2) for _ in range(levels)]
    ops, driven, out, slots, vectors, inside, stars = refs

    def load(base, at):
        return [inside[base + i, at, :] for i in span]

    for level in range(levels - 1, -1, -1):
        bit = (device[0] >> level) & 1
        own, other = vector_pairs[level]
        place_pair(bit, own, other, vectors, range(z.v), range(z.v, 2 * z.v))
        for part in range(z.parts):
            at = pl.ds(part * z.chunk, z.chunk)
            fa, hb = [[vectors[k * z.v + i, at, :] for i in span] for k in range(2)]
            if level == levels - 1:
                back = plus(hb, matvec(lambda i, j: outer[part][i * z.v + j], fa))
                zero = [jnp.zeros_like(value) for value in fa]
                xa, ya, xb, yb = zero, back, fa, zero
            else:
                own, other = inner_maps[level]
                place_pair(bit, own[part], other[part], slots, range(vv), range(vv, 3 * vv))

                def apply(base, vector):
                    return matvec(lambda i, j: slots[base + i * z.v + j], vector)

                xa, yb = load(0, at), load(z.v, at)
                xb = plus(fa, apply(0, xa))
                ya = plus(plus(hb, apply(vv, xb)), apply(2 * vv, yb))
            for i in span:
                inside[i, at, :] = jnp.where(bit == 0, xa[i], xb[i])
                inside[z.v + i, at, :] = jnp.where(bit == 0, ya[i], yb[i])

    x = [inside[i] for i in span]
    y = [inside[z.v + i] for i in span]
    for r in range(z.rows):
        x = plus([driven[r, i] for i in span], matvec(lambda i, j: ops[r, i * z.v + j], x))
        for i in span:
            stars[r, i] = x[i]
    for r in range(z.rows - 1, -1, -1):
        y = plus(
            [stars[r, i] for i in span], matvec(lambda i, j: ops[r, vv + i * z.v + j], y)
        )
        for i in span:
            out[i, pl.ds(r, z.cells, stride=z.rows), :] = y[i]


def trig_tables(z):
    q = np.arange(z.width)[:, None]
    k = (np.arange(z.n)[:, None] + z.n * np.arange(z.per)[None, :]).reshape(1, z.n, 1, z.per)
    angle = 2 * np.pi * ((q.reshape(-1, 1, 1, 1) * k) % z.points) / z.points
    values = np.concatenate([np.cos(angle), np.sin(angle)], axis=2).reshape(z.width, -1)
    high = values.astype(np.float32).astype(ml_dtypes.bfloat16)
    low = (values - high.astype(np.float64)).astype(np.float32).astype(ml_dtypes.bfloat16)
    return high, low


def exchange(value, span, level, both=True):
    pairs = [(d ^ (1 << level), d) for d in range(span) if both or not (d >> level) & 1]
    return lax.ppermute(value, "span", pairs)


def body(residual, inverse_diagonal, prior_increment, coupling, characteristic, cutoffs):
    pitch, span = lax.axis_size("pitch"), lax.axis_size("span")
    z = Sizes(residual, characteristic, pitch)
    vv = z.vv
    levels = span.bit_length() - 1
    residual_t = to_tiles(residual, z)
    prior_t = to_tiles(prior_increment, z)
    diag_t = to_tiles(inverse_diagonal, z)
    couple = jnp.transpose(coupling, (1, 0, 2))
    char = jnp.transpose(characteristic, (0, 3, 4, 1, 2)).reshape(-1, 2, z.harmonics)
    device = lax.axis_index("span").astype(jnp.int32).reshape(1)
    cell, part_cell = (z.cells, LANES), (z.chunk, LANES)
    field = (z.v, z.axial * z.block, LANES)
    scratch = pltpu.VMEM

    payload = call(
        functools.partial(payload_kernel, z),
        [(z.planes + z.rows, LANES)],
        (residual_t, prior_t),
        [HBM] * 2,
        [scratch(field, F32), pltpu.SemaphoreType.DMA((2 * z.v + 1,))],
    )[0]
    blocks = [payload]
    for j in range(1, pitch):
        pairs = [((e + j) % pitch, e) for e in range(pitch)]
        blocks.append(lax.ppermute(payload, "pitch", pairs))

    ops, *maps = call(
        functools.partial(maps_kernel, z),
        [(z.rows, 3 * vv) + cell] + [(3 * vv,) + part_cell] * z.parts,
        (diag_t, couple, payload),
        [HBM, HBM, ANY],
        [
            scratch((3 * vv,) + cell, F32),
            scratch((z.rows, vv) + cell, F32),
            scratch(diag_t.shape, F32),
            scratch(couple.shape, F32),
            scratch((2 * vv,) + cell, F32),
            pltpu.SemaphoreType.DMA((2,)),
        ],
        flops=10_000_000,
    )
    map_levels = []
    for level in range(levels):
        last = level == levels - 1
        others = []
        for value in maps:
            others.append(exchange(value, span, level, not last))
        map_levels.append((maps, others))
        if last:
            break
        count = vv if level == levels - 2 else 3 * vv
        maps = [
            call(
                functools.partial(merge_maps_kernel, z, level, level == levels - 2),
                [(count,) + part_cell],
                (device, mine, other),
                [SMEM, VMEM, VMEM],
                [scratch((6 * vv,) + part_cell, F32)],
            )[0]
            for mine, other in zip(maps, others)
        ]

    high, low = trig_tables(z)
    source, spec, high, low, couple = call(
        functools.partial(prepare_kernel, z),
        [field, (2, 2 * vv, z.harmonics), (high.shape, BF16), (low.shape, BF16), couple.shape],
        (
            residual_t,
            prior_t,
            char,
            jnp.asarray(high),
            jnp.asarray(low),
            couple,
            cutoffs,
            payload,
        ),
        [HBM] * 7 + [ANY],
        [
            scratch(field, F32),
            scratch(field, F32),
            scratch(char.shape, F32),
            pltpu.SMEM(cutoffs.shape, jnp.int32),
            pltpu.SemaphoreType.DMA((7,)),
        ],
        flops=5_000_000,
    )

    rows = 2 * z.v * z.rows
    driven, vectors = call(
        functools.partial(spectral_kernel, z),
        [(z.rows, z.v) + cell, (2 * z.v,) + cell],
        (*blocks, high, low, spec, ops, source, couple),
        [VMEM] * (z.n + 6),
        [
            scratch((rows, z.harmonics), F32),
            scratch((rows, z.harmonics), F32),
            scratch(field, F32),
        ],
        flops=10_000_000,
    )

    vector_levels = []
    for level in range(levels):
        other = exchange(vectors, span, level)
        vector_levels.append((vectors, other))
        if level + 1 < levels:
            mine, others = map_levels[level]
            vectors = call(
                functools.partial(merge_vectors_kernel, z, level),
                [(2 * z.v,) + cell],
                (device, *mine, *others, vectors, other),
                [SMEM] + [VMEM] * (2 * z.parts + 2),
                [scratch((3 * vv,) + part_cell, F32), scratch((4 * z.v,) + cell, F32)],
            )[0]

    arrays = []
    for mine, others in map_levels[:-1]:
        arrays += [*mine, *others]
    arrays += map_levels[-1][1]
    for pair in vector_levels:
        arrays += pair
    update = call(
        functools.partial(final_kernel, z, levels),
        [field],
        (device, *arrays, ops, driven),
        [SMEM] + [VMEM] * (len(arrays) + 2),
        [
            scratch((3 * vv,) + part_cell, F32),
            scratch((2 * z.v,) + cell, F32),
            scratch((2 * z.v,) + cell, F32),
            scratch((z.rows, z.v) + cell, F32),
        ],
        flops=2_000_000,
    )[0]
    return from_tiles(update, z)


def solution(mesh):
    in_specs = (
        P(None, None, "span", "pitch"),
        P(None, None, None, "span", "pitch"),
        P(None, None, "span", "pitch"),
        P(),
        P(),
        P(),
    )
    out_specs = P(None, None, "span", "pitch")
    return jax.shard_map(body, mesh=mesh, in_specs=in_specs, out_specs=out_specs, check_vma=False)
```

```python
import functools

import jax
import jax.numpy as jnp
import ml_dtypes
import numpy as np
from jax import lax
from jax.experimental import pallas as pl
from jax.experimental.pallas import tpu as pltpu
from jax.sharding import PartitionSpec as P


LANES = 128
HALF = 64
VMEM = pl.BlockSpec(memory_space=pltpu.VMEM)
SMEM = pl.BlockSpec(memory_space=pltpu.SMEM)
HBM = pl.BlockSpec(memory_space=pltpu.HBM)
ANY = pl.BlockSpec(memory_space=pl.ANY)
PARTS = 1
MIRRORED = True
F32 = jnp.float32
BF16 = jnp.bfloat16


def call(kernel, outs, ins, specs, scratch=(), flops=1_000_000):
    moved = 4 * sum(int(np.prod(a.shape)) for a in ins)
    ins = [
        pltpu.with_memory_space_constraint(a, pltpu.HBM) if spec is HBM else a
        for a, spec in zip(ins, specs)
    ]
    return kernel_call(kernel, outs, ins, specs, scratch, flops, moved)


def kernel_call(kernel, outs, ins, specs, scratch, flops, moved):
    return pl.pallas_call(
        kernel,
        out_shape=[
            jax.ShapeDtypeStruct(*s) if isinstance(s[0], tuple) else jax.ShapeDtypeStruct(s, F32)
            for s in outs
        ],
        in_specs=list(specs),
        out_specs=[VMEM] * len(outs),
        scratch_shapes=list(scratch),
        cost_estimate=pl.CostEstimate(flops=flops, bytes_accessed=moved, transcendentals=0),
        compiler_params=pltpu.CompilerParams(vmem_limit_bytes=12 * 1024 * 1024),
    )(*ins)


def total(terms):
    terms = list(terms)
    while len(terms) > 1:
        paired = [a + b for a, b in zip(terms[::2], terms[1::2])]
        terms = paired + terms[2 * len(paired) :]
    return terms[0]


def matvec(get, vector):
    size = len(vector)
    return [total([get(i, j) * vector[j] for j in range(size)]) for i in range(size)]


def plus(a, b):
    return [x + y for x, y in zip(a, b)]


def split(x):
    high = x.astype(BF16)
    return high, (x - high.astype(F32)).astype(BF16)


def splat(coupling, which, i, j, shape):
    return jnp.broadcast_to(coupling[i, which : which + 1, j : j + 1], shape)


class Sizes:
    def __init__(self, residual, characteristic, pitch):
        self.v, self.axial, self.rows, self.width = residual.shape
        self.tiles = self.width // LANES
        self.block = self.tiles * self.rows
        self.cells = self.axial * self.tiles
        self.n = pitch
        self.points = pitch * self.width
        self.harmonics = characteristic.shape[2]
        self.per = self.harmonics // pitch
        self.planes = 2 * self.v * self.block
        self.vv = self.v * self.v
        self.parts = PARTS
        self.chunk = self.cells // self.parts


def to_tiles(array, sizes):
    lead = array.shape[:-3]
    array = array.reshape(lead + (sizes.axial, sizes.rows, sizes.tiles, LANES))
    array = jnp.swapaxes(array, -3, -2)
    return array.reshape((-1, sizes.axial * sizes.block, LANES))


def from_tiles(array, sizes):
    array = array.reshape((sizes.v, sizes.axial, sizes.tiles, sizes.rows, LANES))
    array = jnp.swapaxes(array, -3, -2)
    return array.reshape((sizes.v, sizes.axial, sizes.rows, sizes.width))


def opening_kernel(z, *refs):
    ins, refs = refs[:4], refs[4:]
    residual, prior, coupling, payload, ops = refs[:5]
    outs, (maps, powers, diag, splats, sems) = refs[5 : 5 + z.parts], refs[5 + z.parts :]
    held = [coupling, diag, prior, residual]
    copies = [
        pltpu.make_async_copy(a, b, sems.at[k]) for k, (a, b) in enumerate(zip(ins, held))
    ]
    for copy in copies:
        copy.start()
    span = range(z.v)
    vv = z.vv

    copies[0].wait()
    for which in range(2):
        for i in span:
            for j in span:
                splats[which * vv + i * z.v + j] = -splat(
                    coupling, which, i, j, (z.cells, LANES)
                )
    copies[2].wait()
    lane = lax.broadcasted_iota(jnp.int32, (z.rows, LANES), 1)
    halo = jnp.zeros((z.rows, LANES), F32)
    for v in span:
        for a in range(z.axial):
            first = prior[v, pl.ds(a * z.block, z.rows), :][:, 0:1]
            last = prior[v, pl.ds((a + 1) * z.block - z.rows, z.rows), :][:, LANES - 1 :]
            halo = jnp.where(lane == v * z.axial + a, first, halo)
            halo = jnp.where(lane == HALF + v * z.axial + a, last, halo)
    payload[pl.ds(z.planes, z.rows), :] = halo
    copies[3].wait()
    for q, a in enumerate((0, z.axial - 1)):
        for v in span:
            payload[pl.ds((q * z.v + v) * z.block, z.block), :] = residual[
                v, pl.ds(a * z.block, z.block), :
            ]
    copies[1].wait()

    def operators(r, _):
        for i in span:
            d = [diag[i * z.v + j, pl.ds(r, z.cells, stride=z.rows), :] for j in span]
            for k in span:
                for which in range(2):
                    ops[r, which * vv + i * z.v + k] = total(
                        [d[j] * splats[which * vv + j * z.v + k] for j in span]
                    )
                ops[r, 2 * vv + i * z.v + k] = d[k]
        return 0

    lax.fori_loop(0, z.rows, operators, 0)

    for m in range(vv):
        powers[0, m] = ops[0, m]

    def forward(r, _):
        for k in span:
            column = [powers[r - 1, j * z.v + k] for j in span]
            new = matvec(lambda i, j: ops[r, i * z.v + j], column)
            for i in span:
                powers[r, i * z.v + k] = new[i]
        return 0

    lax.fori_loop(1, z.rows, forward, 0)
    top = z.rows - 1
    for m in range(vv):
        maps[m] = powers[top, m]
        maps[vv + m] = powers[top, m]
        maps[2 * vv + m] = ops[top, vv + m]

    def backward(step, _):
        r = top - step
        for k in span:
            for base in (vv, 2 * vv):
                column = [maps[base + j * z.v + k] for j in span]
                new = matvec(lambda i, j: ops[r, vv + i * z.v + j], column)
                for i in span:
                    value = new[i]
                    if base == vv:
                        value = value + powers[r, i * z.v + k]
                    maps[base + i * z.v + k] = value
        return 0

    lax.fori_loop(1, z.rows, backward, 0)
    for part in range(z.parts):
        for m in range(3 * vv):
            outs[part][m] = maps[m, pl.ds(part * z.chunk, z.chunk), :]


def prepare_kernel(z, prior, residual, coupling, *refs):
    ins, refs = refs[:4], refs[4:]
    source, spec, splats, table_high, table_low, char, cutoffs, sems = refs
    held = [char, cutoffs, table_high, table_low]
    copies = [
        pltpu.make_async_copy(a, b, sems.at[k]) for k, (a, b) in enumerate(zip(ins, held))
    ]
    for copy in copies:
        copy.start()
    span = range(z.v)
    vv = z.vv
    shape = (z.rows, LANES)
    factors = {
        (which, i, j): splat(coupling, which, i, j, shape)
        for which in range(2, 6)
        for i in span
        for j in span
    }
    for which in range(2, 4):
        for i in span:
            for j in span:
                splats[(which - 2) * vv + i * z.v + j] = factors[which, i, j]

    def scalar(which, i, j):
        return factors[which, i, j]

    lane = lax.broadcasted_iota(jnp.int32, (z.rows, LANES), 1)

    def tile(ref, v, a, h):
        return ref[v, pl.ds(a * z.block + h * z.rows, z.rows), :]

    for a in range(z.axial):
        here = [[tile(prior, v, a, h) for h in range(z.tiles)] for v in span]
        up = [[pltpu.roll(x, 1, 1) for x in row] for row in here]
        down = [[pltpu.roll(x, LANES - 1, 1) for x in row] for row in here]
        for h in range(z.tiles):
            lower, upper = [], []
            for v in span:
                edge = up[v][h - 1] if h else jnp.zeros((z.rows, LANES), F32)
                lower.append(jnp.where(lane == 0, edge, up[v][h]))
                edge = down[v][h + 1] if h + 1 < z.tiles else jnp.zeros((z.rows, LANES), F32)
                upper.append(jnp.where(lane == LANES - 1, edge, down[v][h]))
            terms = [(2, lower), (3, upper)]
            if a > 0:
                terms.append((4, [tile(prior, v, a - 1, h) for v in span]))
            if a + 1 < z.axial:
                terms.append((5, [tile(prior, v, a + 1, h) for v in span]))
            for i in span:
                value = tile(residual, i, a, h)
                for which, field in terms:
                    value = value - total([field[j] * scalar(which, i, j) for j in span])
                source[i, pl.ds(a * z.block + h * z.rows, z.rows), :] = value

    place = lax.broadcasted_iota(jnp.int32, (1, z.harmonics), 1)
    harmonic = (place % z.per) * z.n + place // z.per
    k_of = lax.broadcasted_iota(jnp.int32, (z.harmonics, z.harmonics), 0)
    select = jnp.where(k_of == harmonic, 1.0, 0.0).astype(BF16)
    for copy in copies[:2]:
        copy.wait()
    value = jnp.concatenate([char[:, c, :] for c in range(2)], axis=0)
    high = value.astype(BF16)
    middle, low = split(value - high.astype(F32))
    ordered = total(
        [jnp.dot(part, select, preferred_element_type=F32) for part in (high, middle, low)]
    )
    weight = jnp.where(harmonic == 0, 1.0, 2.0) / z.points
    for q in range(2):
        factor = jnp.where(harmonic < cutoffs[:, q : q + 1], weight, 0.0)
        for c in range(2):
            first = (2 * c + q) * vv
            spec[c, pl.ds(q * vv, vv), :] = ordered[first : first + vv] * factor
    for copy in copies[2:]:
        copy.wait()


def spectral_kernel(z, *refs):
    blocks = refs[: z.n]
    table_high, table_low, spec, ops, source, splats, driven, vectors, real, imag, total_source = (
        refs[z.n :]
    )
    span = range(z.v)
    vv = z.vv
    flat = 2 * z.v * z.rows

    def scalar(which, i, j):
        return splats[(which - 2) * vv + i * z.v + j]

    def column(halo, at):
        return jnp.broadcast_to(halo[:, at : at + 1], (z.rows, LANES))

    def plane(ref):
        value = ref[pl.ds(0, z.planes), :].reshape(2 * z.v, z.tiles, z.rows, LANES)
        parts = [value[:, h].reshape(flat, LANES) for h in range(z.tiles)]
        return parts[0] if len(parts) == 1 else jnp.concatenate(parts, axis=1)

    x = [plane(ref) for ref in blocks]

    def combine(coefficients):
        terms = []
        for c, value in zip(coefficients, x):
            if abs(c) < 1e-12:
                continue
            if abs(c - 1) < 1e-12:
                terms.append(value)
            elif abs(c + 1) < 1e-12:
                terms.append(-value)
            else:
                terms.append(value * float(c))
        return total(terms) if terms else None

    def table(ref, s):
        return ref[:, pl.ds(2 * z.per * s, 2 * z.per)]

    turns = 2 * np.pi * np.arange(z.n) / z.n
    for s in range(z.n // 2 + 1):
        yr = combine(np.cos(turns * s))
        yi = combine(-np.sin(turns * s))
        highs, lows = zip(*[split(y) for y in (yr, yi) if y is not None])
        both = jnp.concatenate(highs + lows, axis=0)
        high = jnp.concatenate(highs, axis=0) if len(highs) > 1 else highs[0]
        rows = high.shape[0]
        for t in sorted({s, (z.n - s) % z.n}):
            first = jnp.dot(both, table(table_high, t), preferred_element_type=F32)
            second = jnp.dot(high, table(table_low, t), preferred_element_type=F32)
            y = first[:rows] + first[rows:] + second
            re, im = y[:flat, : z.per], -y[:flat, z.per :]
            if yi is not None:
                sign = 1.0 if t == s else -1.0
                re = re + sign * y[flat:, z.per :]
                im = im + sign * y[flat:, : z.per]
            real[:, pl.ds(z.per * t, z.per)] = re
            imag[:, pl.ds(z.per * t, z.per)] = im

    out_real, out_imag = [], []
    for q in range(2):
        rows = [pl.ds((q * z.v + j) * z.rows, z.rows) for j in span]
        re = [real[at, :] for at in rows]
        im = [imag[at, :] for at in rows]
        for i in span:
            base = (q * z.v + i) * z.v
            cr = [spec[0, pl.ds(base + j, 1), :] for j in span]
            ci = [spec[1, pl.ds(base + j, 1), :] for j in span]
            out_real.append(total([cr[j] * re[j] - ci[j] * im[j] for j in span]))
            out_imag.append(total([cr[j] * im[j] + ci[j] * re[j] for j in span]))
    cr = jnp.concatenate(out_real, axis=0)
    ci = -jnp.concatenate(out_imag, axis=0)
    parts = []
    for s in range(z.n):
        at = slice(s * z.per, (s + 1) * z.per)
        parts += [cr[:, at], ci[:, at]]
    high, low = split(jnp.concatenate(parts, axis=1))
    dims = (((1,), (1,)), ((), ()))
    both = jnp.concatenate([high, low], axis=0)
    first = lax.dot_general(both, table_high[...], dims, preferred_element_type=F32)
    second = lax.dot_general(high, table_low[...], dims, preferred_element_type=F32)
    correction = first[:flat] + first[flat:] + second

    lane = lax.broadcasted_iota(jnp.int32, (z.rows, LANES), 1)
    before = blocks[z.n - 1][pl.ds(z.planes, z.rows), :]
    after = blocks[1][pl.ds(z.planes, z.rows), :]
    for a in range(z.axial):
        lows = [column(before, HALF + v * z.axial + a) for v in span]
        highs = [column(after, v * z.axial + a) for v in span]
        for h in range(z.tiles):
            at = pl.ds(a * z.block + h * z.rows, z.rows)
            for i in span:
                value = source[i, at, :]
                if h == 0:
                    edge = total([lows[j] * scalar(2, i, j) for j in span])
                    value = value - jnp.where(lane == 0, edge, 0.0)
                if h == z.tiles - 1:
                    edge = total([highs[j] * scalar(3, i, j) for j in span])
                    value = value - jnp.where(lane == LANES - 1, edge, 0.0)
                for q, plane_a in enumerate((0, z.axial - 1)):
                    if a == plane_a:
                        first = (q * z.v + i) * z.rows
                        value = value + correction[
                            first : first + z.rows, h * LANES : (h + 1) * LANES
                        ]
                total_source[i, at, :] = value

    stars = []
    for r in range(z.rows):
        row = [total_source[j, pl.ds(r, z.cells, stride=z.rows), :] for j in span]
        new = matvec(lambda i, j: ops[r, 2 * vv + i * z.v + j], row)
        for i in span:
            driven[r, i] = new[i]
        if r:
            new = plus(new, matvec(lambda i, j: ops[r, i * z.v + j], stars[-1]))
        stars.append(new)
    back = stars[-1]
    for r in range(z.rows - 2, -1, -1):
        back = plus(stars[r], matvec(lambda i, j: ops[r, vv + i * z.v + j], back))
    for i in span:
        vectors[i] = stars[-1][i]
        vectors[z.v + i] = back[i]


def place_pair(where, own, other, slots, lower, upper):
    def fill(a, b):
        for k, m in enumerate(lower):
            slots[k] = a[m]
        for k, m in enumerate(upper):
            slots[len(lower) + k] = b[m]

    @pl.when(where == 0)
    def _():
        fill(own, other)

    @pl.when(where != 0)
    def _():
        fill(other, own)


def merge_maps_kernel(z, level, device, own, other, out, slots):
    vv = z.vv
    every = list(range(3 * vv))
    place_pair((device[0] >> level) & 1, own, other, slots, every, every)
    span = range(z.v)

    def column(base, k):
        return [slots[base + j * z.v + k] for j in span]

    def apply(base, vector):
        return matvec(lambda i, j: slots[base + i * z.v + j], vector)

    up = 3 * vv
    for k in span:
        state = column(0, k)
        back = plus(column(vv, k), apply(2 * vv, apply(up + vv, state)))
        state = apply(up, state)
        through = apply(2 * vv, column(up + 2 * vv, k))
        for i in span:
            out[i * z.v + k] = state[i]
            out[vv + i * z.v + k] = back[i]
            out[2 * vv + i * z.v + k] = through[i]


def merge_last_kernel(z, level, device, *refs):
    own_maps, other_maps = refs[: z.parts], refs[z.parts : 2 * z.parts]
    own, other, out, state_out, slots, vectors = refs[2 * z.parts :]
    vv = z.vv
    span = range(z.v)
    bit = (device[0] >> level) & 1
    half = (device[0] >> (level + 1)) & 1
    every = list(range(2 * z.v))
    place_pair(bit, own, other, vectors, every, every)
    lower, upper = range(3 * vv), range(2 * vv)
    for part in range(z.parts):
        at = pl.ds(part * z.chunk, z.chunk)
        place_pair(bit, own_maps[part], other_maps[part], slots, lower, upper)

        def apply(base, vector):
            return matvec(lambda i, j: slots[base + i * z.v + j], vector)

        fa, ha, fb, hb = [[vectors[k * z.v + i, at, :] for i in span] for k in range(4)]
        state = plus(fb, apply(3 * vv, fa))
        back = plus(ha, apply(2 * vv, plus(hb, apply(4 * vv, fa))))
        for i in span:
            state_out[i, at, :] = state[i]
            out[i, at, :] = jnp.where(half == 0, state[i], back[i])
        for k in span:
            column = [slots[j * z.v + k] for j in span]
            column = apply(2 * vv, apply(4 * vv, column))
            for i in span:
                out[z.v + i * z.v + k, at, :] = slots[vv + i * z.v + k] + column[i]


def merge_vectors_kernel(z, level, device, *refs):
    own_maps, other_maps = refs[: z.parts], refs[z.parts : 2 * z.parts]
    own, other, out, slots, vectors = refs[2 * z.parts :]
    vv = z.vv
    span = range(z.v)
    bit = (device[0] >> level) & 1
    every = list(range(2 * z.v))
    place_pair(bit, own, other, vectors, every, every)
    for part in range(z.parts):
        at = pl.ds(part * z.chunk, z.chunk)
        place_pair(
            bit, own_maps[part], other_maps[part], slots, range(2 * vv, 3 * vv), range(2 * vv)
        )

        def apply(base, vector):
            return matvec(lambda i, j: slots[base + i * z.v + j], vector)

        fa, ha, fb, hb = [[vectors[k * z.v + i, at, :] for i in span] for k in range(4)]
        state = plus(fb, apply(vv, fa))
        back = plus(ha, apply(0, plus(hb, apply(2 * vv, fa))))
        for i in span:
            out[i, at, :] = state[i]
            out[z.v + i, at, :] = back[i]


def final_kernel(z, levels, device, *refs):
    span = range(z.v)
    vv = z.vv
    refs = list(refs)

    def take(count):
        taken = refs[:count]
        del refs[:count]
        return taken

    inner_maps = [(take(z.parts), take(z.parts)) for _ in range(levels - 1)]
    vector_pairs = [take(2) for _ in range(levels - 1)]
    own_state, told, ops, driven, out, slots, vectors, inside, stars = refs

    def load(base, at):
        return [inside[base + i, at, :] for i in span]

    half = (device[0] >> (levels - 1)) & 1
    word = [told[i] for i in span]
    back = matvec(lambda i, j: told[z.v + i * z.v + j], [own_state[i] for i in span])
    for i in span:
        zero = jnp.zeros_like(word[i])
        inside[i] = jnp.where(half == 0, zero, word[i])
        inside[z.v + i] = jnp.where(half == 0, word[i] + back[i], zero)

    for level in range(levels - 2, -1, -1):
        bit = (device[0] >> level) & 1
        own, other = vector_pairs[level]
        place_pair(bit, own, other, vectors, range(z.v), range(z.v, 2 * z.v))
        for part in range(z.parts):
            at = pl.ds(part * z.chunk, z.chunk)
            fa, hb = [[vectors[k * z.v + i, at, :] for i in span] for k in range(2)]
            own, other = inner_maps[level]
            place_pair(bit, own[part], other[part], slots, range(vv), range(vv, 3 * vv))

            def apply(base, vector):
                return matvec(lambda i, j: slots[base + i * z.v + j], vector)

            xa, yb = load(0, at), load(z.v, at)
            xb = plus(fa, apply(0, xa))
            ya = plus(plus(hb, apply(vv, xb)), apply(2 * vv, yb))
            for i in span:
                inside[i, at, :] = jnp.where(bit == 0, xa[i], xb[i])
                inside[z.v + i, at, :] = jnp.where(bit == 0, ya[i], yb[i])

    x = [inside[i] for i in span]
    y = [inside[z.v + i] for i in span]
    for r in range(z.rows):
        x = plus([driven[r, i] for i in span], matvec(lambda i, j: ops[r, i * z.v + j], x))
        for i in span:
            stars[r, i] = x[i]
    for r in range(z.rows - 1, -1, -1):
        y = plus(
            [stars[r, i] for i in span], matvec(lambda i, j: ops[r, vv + i * z.v + j], y)
        )
        for i in span:
            out[i, pl.ds(r, z.cells, stride=z.rows), :] = y[i]


def trig_tables(z):
    q = np.arange(z.width)[:, None]
    k = (np.arange(z.n)[:, None] + z.n * np.arange(z.per)[None, :]).reshape(1, z.n, 1, z.per)
    angle = 2 * np.pi * ((q.reshape(-1, 1, 1, 1) * k) % z.points) / z.points
    values = np.concatenate([np.cos(angle), np.sin(angle)], axis=2).reshape(z.width, -1)
    high = values.astype(np.float32).astype(ml_dtypes.bfloat16)
    low = (values - high.astype(np.float64)).astype(np.float32).astype(ml_dtypes.bfloat16)
    return high, low


def exchange(value, span, level, mirrored=False):
    flip = (2 << level) - 2 if mirrored else 1 << level
    return lax.ppermute(value, "span", [(d ^ flip, d) for d in range(span)])


def body(residual, inverse_diagonal, prior_increment, coupling, characteristic, cutoffs):
    pitch, span = lax.axis_size("pitch"), lax.axis_size("span")
    z = Sizes(residual, characteristic, pitch)
    vv = z.vv
    levels = span.bit_length() - 1
    residual_t = to_tiles(residual, z)
    prior_t = to_tiles(prior_increment, z)
    diag_t = to_tiles(inverse_diagonal, z)
    couple = jnp.transpose(coupling, (1, 0, 2))
    char = jnp.transpose(characteristic, (0, 3, 4, 1, 2)).reshape(-1, 2, z.harmonics)
    device = lax.axis_index("span").astype(jnp.int32).reshape(1)
    cell, part_cell = (z.cells, LANES), (z.chunk, LANES)
    field = (z.v, z.axial * z.block, LANES)
    scratch = pltpu.VMEM

    high, low = [jnp.asarray(table) for table in trig_tables(z)]
    residual_t, prior_t, couple, payload, ops, *maps = call(
        functools.partial(opening_kernel, z),
        [field, field, couple.shape, (z.planes + z.rows, LANES), (z.rows, 3 * vv) + cell]
        + [(3 * vv,) + part_cell] * z.parts,
        (couple, diag_t, prior_t, residual_t),
        [HBM] * 4,
        [
            scratch((3 * vv,) + cell, F32),
            scratch((z.rows, vv) + cell, F32),
            scratch(diag_t.shape, F32),
            scratch((2 * vv,) + cell, F32),
            pltpu.SemaphoreType.DMA((4,)),
        ],
        flops=10_000_000,
    )
    blocks = [payload]
    for j in range(1, pitch):
        pairs = [((e + j) % pitch, e) for e in range(pitch)]
        blocks.append(lax.ppermute(payload, "pitch", pairs))

    map_levels = []
    for level in range(levels - 1):
        others = []
        for value in maps:
            others.append(exchange(value, span, level))
        map_levels.append((maps, others))
        if level + 2 < levels:
            maps = [
                call(
                    functools.partial(merge_maps_kernel, z, level),
                    [(3 * vv,) + part_cell],
                    (device, mine, other),
                    [SMEM, VMEM, VMEM],
                    [scratch((6 * vv,) + part_cell, F32)],
                )[0]
                for mine, other in zip(maps, others)
            ]

    source, spec, splats, high, low = call(
        functools.partial(prepare_kernel, z),
        [
            field,
            (2, 2 * vv, z.harmonics),
            (2 * vv, z.rows, LANES),
            (high.shape, BF16),
            (low.shape, BF16),
        ],
        (prior_t, residual_t, couple, char, cutoffs.reshape(1, 2), high, low),
        [VMEM] * 3 + [HBM] * 4,
        [
            scratch(char.shape, F32),
            scratch((1, 2), jnp.int32),
            pltpu.SemaphoreType.DMA((4,)),
        ],
        flops=5_000_000,
    )

    rows = 2 * z.v * z.rows
    driven, vectors = call(
        functools.partial(spectral_kernel, z),
        [(z.rows, z.v) + cell, (2 * z.v,) + cell],
        (*blocks, high, low, spec, ops, source, splats),
        [VMEM] * (z.n + 6),
        [
            scratch((rows, z.harmonics), F32),
            scratch((rows, z.harmonics), F32),
            scratch(field, F32),
        ],
        flops=10_000_000,
    )

    vector_levels = []
    for level in range(levels - 1):
        other = exchange(vectors, span, level)
        vector_levels.append((vectors, other))
        mine, others = map_levels[level]
        ins = (device, *mine, *others, vectors, other)
        specs = [SMEM] + [VMEM] * (2 * z.parts + 2)
        if level + 2 < levels:
            vectors = call(
                functools.partial(merge_vectors_kernel, z, level),
                [(2 * z.v,) + cell],
                ins,
                specs,
                [scratch((3 * vv,) + part_cell, F32), scratch((4 * z.v,) + cell, F32)],
            )[0]
        else:
            tell, state = call(
                functools.partial(merge_last_kernel, z, level),
                [(z.v + vv,) + cell, (z.v,) + cell],
                ins,
                specs,
                [scratch((5 * vv,) + part_cell, F32), scratch((4 * z.v,) + cell, F32)],
            )
    told = exchange(tell, span, levels - 1, MIRRORED)

    arrays = []
    for mine, others in map_levels:
        arrays += [*mine, *others]
    for pair in vector_levels:
        arrays += pair
    arrays += [state, told]
    update = call(
        functools.partial(final_kernel, z, levels),
        [field],
        (device, *arrays, ops, driven),
        [SMEM] + [VMEM] * (len(arrays) + 2),
        [
            scratch((3 * vv,) + part_cell, F32),
            scratch((2 * z.v,) + cell, F32),
            scratch((2 * z.v,) + cell, F32),
            scratch((z.rows, z.v) + cell, F32),
        ],
        flops=2_000_000,
    )[0]
    return from_tiles(update, z)


def solution(mesh):
    in_specs = (
        P(None, None, "span", "pitch"),
        P(None, None, None, "span", "pitch"),
        P(None, None, "span", "pitch"),
        P(),
        P(),
        P(),
    )
    out_specs = P(None, None, "span", "pitch")
    return jax.shard_map(body, mesh=mesh, in_specs=in_specs, out_specs=out_specs, check_vma=False)
```

```python
import functools

import jax
import jax.numpy as jnp
import ml_dtypes
import numpy as np
from jax import lax
from jax.experimental import pallas as pl
from jax.experimental.pallas import tpu as pltpu
from jax.sharding import PartitionSpec as P


LANES = 128
HALF = 64
VMEM = pl.BlockSpec(memory_space=pltpu.VMEM)
SMEM = pl.BlockSpec(memory_space=pltpu.SMEM)
HBM = pl.BlockSpec(memory_space=pltpu.HBM)
ANY = pl.BlockSpec(memory_space=pl.ANY)
PARTS = 2
MIRRORED = True
F32 = jnp.float32
BF16 = jnp.bfloat16


def call(kernel, outs, ins, specs, scratch=(), flops=1_000_000):
    moved = 4 * sum(int(np.prod(a.shape)) for a in ins)
    ins = [
        pltpu.with_memory_space_constraint(a, pltpu.HBM) if spec is HBM else a
        for a, spec in zip(ins, specs)
    ]
    return kernel_call(kernel, outs, ins, specs, scratch, flops, moved)


def kernel_call(kernel, outs, ins, specs, scratch, flops, moved):
    return pl.pallas_call(
        kernel,
        out_shape=[
            jax.ShapeDtypeStruct(*s) if isinstance(s[0], tuple) else jax.ShapeDtypeStruct(s, F32)
            for s in outs
        ],
        in_specs=list(specs),
        out_specs=[VMEM] * len(outs),
        scratch_shapes=list(scratch),
        cost_estimate=pl.CostEstimate(flops=flops, bytes_accessed=moved, transcendentals=0),
        compiler_params=pltpu.CompilerParams(vmem_limit_bytes=12 * 1024 * 1024),
    )(*ins)


def total(terms):
    terms = list(terms)
    while len(terms) > 1:
        paired = [a + b for a, b in zip(terms[::2], terms[1::2])]
        terms = paired + terms[2 * len(paired) :]
    return terms[0]


def matvec(get, vector):
    size = len(vector)
    return [total([get(i, j) * vector[j] for j in range(size)]) for i in range(size)]


def plus(a, b):
    return [x + y for x, y in zip(a, b)]


def split(x):
    high = x.astype(BF16)
    return high, (x - high.astype(F32)).astype(BF16)


def splat(coupling, which, i, j, shape):
    return jnp.broadcast_to(coupling[i, which : which + 1, j : j + 1], shape)


class Sizes:
    def __init__(self, residual, characteristic, pitch):
        self.v, self.axial, self.rows, self.width = residual.shape
        self.tiles = self.width // LANES
        self.block = self.tiles * self.rows
        self.cells = self.axial * self.tiles
        self.n = pitch
        self.points = pitch * self.width
        self.harmonics = characteristic.shape[2]
        self.per = self.harmonics // pitch
        self.planes = 2 * self.v * self.block
        self.vv = self.v * self.v
        self.parts = PARTS
        self.chunk = self.cells // self.parts


def to_tiles(array, sizes):
    lead = array.shape[:-3]
    array = array.reshape(lead + (sizes.axial, sizes.rows, sizes.tiles, LANES))
    array = jnp.swapaxes(array, -3, -2)
    return array.reshape((-1, sizes.axial * sizes.block, LANES))


def from_tiles(array, sizes):
    array = array.reshape((sizes.v, sizes.axial, sizes.tiles, sizes.rows, LANES))
    array = jnp.swapaxes(array, -3, -2)
    return array.reshape((sizes.v, sizes.axial, sizes.rows, sizes.width))


def opening_kernel(z, *refs):
    ins, refs = refs[:4], refs[5:]
    residual, prior, coupling, payload, ops = refs[:5]
    outs, (maps, powers, diag, splats, sems) = refs[5 : 5 + z.parts], refs[5 + z.parts :]
    span = range(z.v)
    vv = z.vv
    coupling_h, diag_h, prior_h, residual_h = ins
    pairs = [(coupling_h, coupling), (prior_h, prior), (residual_h, residual)]
    for i in span:
        at = pl.ds(i * z.v, z.v)
        pairs.append((diag_h.at[at], diag.at[at]))
    copies = [pltpu.make_async_copy(a, b, sems.at[k]) for k, (a, b) in enumerate(pairs)]
    for k in (0, 1, 2, 3, 4, 5, 6, 7):
        copies[k].start()

    copies[0].wait()
    for which in range(2):
        for i in span:
            for j in span:
                splats[which * vv + i * z.v + j] = -splat(
                    coupling, which, i, j, (z.cells, LANES)
                )
    copies[1].wait()
    lane = lax.broadcasted_iota(jnp.int32, (z.rows, LANES), 1)
    halo = jnp.zeros((z.rows, LANES), F32)
    for v in span:
        for a in range(z.axial):
            first = prior[v, pl.ds(a * z.block, z.rows), :][:, 0:1]
            last = prior[v, pl.ds((a + 1) * z.block - z.rows, z.rows), :][:, LANES - 1 :]
            halo = jnp.where(lane == v * z.axial + a, first, halo)
            halo = jnp.where(lane == HALF + v * z.axial + a, last, halo)
    payload[pl.ds(z.planes, z.rows), :] = halo
    copies[2].wait()
    for q, a in enumerate((0, z.axial - 1)):
        for v in span:
            payload[pl.ds((q * z.v + v) * z.block, z.block), :] = residual[
                v, pl.ds(a * z.block, z.block), :
            ]

    for i in span:
        copies[3 + i].wait()

        def operators(r, _, i=i):
            d = [diag[i * z.v + j, pl.ds(r, z.cells, stride=z.rows), :] for j in span]
            for k in span:
                for which in range(2):
                    ops[r, which * vv + i * z.v + k] = total(
                        [d[j] * splats[which * vv + j * z.v + k] for j in span]
                    )
                ops[r, 2 * vv + i * z.v + k] = d[k]
            return 0

        lax.fori_loop(0, z.rows, operators, 0, unroll=True)

    for m in range(vv):
        powers[0, m] = ops[0, m]

    def forward(r, _):
        for k in span:
            column = [powers[r - 1, j * z.v + k] for j in span]
            new = matvec(lambda i, j: ops[r, i * z.v + j], column)
            for i in span:
                powers[r, i * z.v + k] = new[i]
        return 0

    lax.fori_loop(1, z.rows, forward, 0, unroll=True)
    top = z.rows - 1
    for m in range(vv):
        maps[m] = powers[top, m]
        maps[vv + m] = powers[top, m]
        maps[2 * vv + m] = ops[top, vv + m]

    def backward(step, _):
        r = top - step
        for k in span:
            for base in (vv, 2 * vv):
                column = [maps[base + j * z.v + k] for j in span]
                new = matvec(lambda i, j: ops[r, vv + i * z.v + j], column)
                for i in span:
                    value = new[i]
                    if base == vv:
                        value = value + powers[r, i * z.v + k]
                    maps[base + i * z.v + k] = value
        return 0

    lax.fori_loop(1, z.rows, backward, 0, unroll=True)
    for part in range(z.parts):
        for m in range(3 * vv):
            outs[part][m] = maps[m, pl.ds(part * z.chunk, z.chunk), :]


def prepare_kernel(z, prior, residual, coupling, *refs):
    ins, refs = refs[:4], refs[4:]
    source, spec, splats, table_high, table_low, char, cutoffs, sems = refs
    held = [char, cutoffs, table_high, table_low]
    copies = [
        pltpu.make_async_copy(a, b, sems.at[k]) for k, (a, b) in enumerate(zip(ins, held))
    ]
    for copy in copies:
        copy.start()
    span = range(z.v)
    vv = z.vv
    shape = (z.rows, LANES)
    factors = {
        (which, i, j): splat(coupling, which, i, j, shape)
        for which in range(2, 6)
        for i in span
        for j in span
    }
    for which in range(2, 4):
        for i in span:
            for j in span:
                splats[(which - 2) * vv + i * z.v + j] = factors[which, i, j]

    def scalar(which, i, j):
        return factors[which, i, j]

    lane = lax.broadcasted_iota(jnp.int32, (z.rows, LANES), 1)

    def tile(ref, v, a, h):
        return ref[v, pl.ds(a * z.block + h * z.rows, z.rows), :]

    for a in range(z.axial):
        here = [[tile(prior, v, a, h) for h in range(z.tiles)] for v in span]
        up = [[pltpu.roll(x, 1, 1) for x in row] for row in here]
        down = [[pltpu.roll(x, LANES - 1, 1) for x in row] for row in here]
        for h in range(z.tiles):
            lower, upper = [], []
            for v in span:
                edge = up[v][h - 1] if h else jnp.zeros((z.rows, LANES), F32)
                lower.append(jnp.where(lane == 0, edge, up[v][h]))
                edge = down[v][h + 1] if h + 1 < z.tiles else jnp.zeros((z.rows, LANES), F32)
                upper.append(jnp.where(lane == LANES - 1, edge, down[v][h]))
            terms = [(2, lower), (3, upper)]
            if a > 0:
                terms.append((4, [tile(prior, v, a - 1, h) for v in span]))
            if a + 1 < z.axial:
                terms.append((5, [tile(prior, v, a + 1, h) for v in span]))
            for i in span:
                value = tile(residual, i, a, h)
                for which, field in terms:
                    value = value - total([field[j] * scalar(which, i, j) for j in span])
                source[i, pl.ds(a * z.block + h * z.rows, z.rows), :] = value

    place = lax.broadcasted_iota(jnp.int32, (1, z.harmonics), 1)
    harmonic = (place % z.per) * z.n + place // z.per
    k_of = lax.broadcasted_iota(jnp.int32, (z.harmonics, z.harmonics), 0)
    select = jnp.where(k_of == harmonic, 1.0, 0.0).astype(BF16)
    for copy in copies[:2]:
        copy.wait()
    value = jnp.concatenate([char[:, c, :] for c in range(2)], axis=0)
    high = value.astype(BF16)
    middle, low = split(value - high.astype(F32))
    ordered = total(
        [jnp.dot(part, select, preferred_element_type=F32) for part in (high, middle, low)]
    )
    weight = jnp.where(harmonic == 0, 1.0, 2.0) / z.points
    for q in range(2):
        factor = jnp.where(harmonic < cutoffs[:, q : q + 1], weight, 0.0)
        for c in range(2):
            first = (2 * c + q) * vv
            spec[c, pl.ds(q * vv, vv), :] = ordered[first : first + vv] * factor
    for copy in copies[2:]:
        copy.wait()


def spectral_kernel(z, *refs):
    blocks = refs[: z.n]
    table_high, table_low, spec, ops, source, splats, driven, vectors, real, imag, total_source = (
        refs[z.n :]
    )
    span = range(z.v)
    vv = z.vv
    flat = 2 * z.v * z.rows

    def scalar(which, i, j):
        return splats[(which - 2) * vv + i * z.v + j]

    def column(halo, at):
        return jnp.broadcast_to(halo[:, at : at + 1], (z.rows, LANES))

    def plane(ref):
        value = ref[pl.ds(0, z.planes), :].reshape(2 * z.v, z.tiles, z.rows, LANES)
        parts = [value[:, h].reshape(flat, LANES) for h in range(z.tiles)]
        return parts[0] if len(parts) == 1 else jnp.concatenate(parts, axis=1)

    x = [plane(ref) for ref in blocks]

    def combine(coefficients):
        terms = []
        for c, value in zip(coefficients, x):
            if abs(c) < 1e-12:
                continue
            if abs(c - 1) < 1e-12:
                terms.append(value)
            elif abs(c + 1) < 1e-12:
                terms.append(-value)
            else:
                terms.append(value * float(c))
        return total(terms) if terms else None

    def table(ref, s):
        return ref[:, pl.ds(2 * z.per * s, 2 * z.per)]

    turns = 2 * np.pi * np.arange(z.n) / z.n
    for s in range(z.n // 2 + 1):
        yr = combine(np.cos(turns * s))
        yi = combine(-np.sin(turns * s))
        highs, lows = zip(*[split(y) for y in (yr, yi) if y is not None])
        both = jnp.concatenate(highs + lows, axis=0)
        high = jnp.concatenate(highs, axis=0) if len(highs) > 1 else highs[0]
        rows = high.shape[0]
        for t in sorted({s, (z.n - s) % z.n}):
            first = jnp.dot(both, table(table_high, t), preferred_element_type=F32)
            second = jnp.dot(high, table(table_low, t), preferred_element_type=F32)
            y = first[:rows] + first[rows:] + second
            re, im = y[:flat, : z.per], -y[:flat, z.per :]
            if yi is not None:
                sign = 1.0 if t == s else -1.0
                re = re + sign * y[flat:, z.per :]
                im = im + sign * y[flat:, : z.per]
            real[:, pl.ds(z.per * t, z.per)] = re
            imag[:, pl.ds(z.per * t, z.per)] = im

    out_real, out_imag = [], []
    for q in range(2):
        rows = [pl.ds((q * z.v + j) * z.rows, z.rows) for j in span]
        re = [real[at, :] for at in rows]
        im = [imag[at, :] for at in rows]
        for i in span:
            base = (q * z.v + i) * z.v
            cr = [spec[0, pl.ds(base + j, 1), :] for j in span]
            ci = [spec[1, pl.ds(base + j, 1), :] for j in span]
            out_real.append(total([cr[j] * re[j] - ci[j] * im[j] for j in span]))
            out_imag.append(total([cr[j] * im[j] + ci[j] * re[j] for j in span]))
    cr = jnp.concatenate(out_real, axis=0)
    ci = -jnp.concatenate(out_imag, axis=0)
    parts = []
    for s in range(z.n):
        at = slice(s * z.per, (s + 1) * z.per)
        parts += [cr[:, at], ci[:, at]]
    high, low = split(jnp.concatenate(parts, axis=1))
    dims = (((1,), (1,)), ((), ()))
    both = jnp.concatenate([high, low], axis=0)
    first = lax.dot_general(both, table_high[...], dims, preferred_element_type=F32)
    second = lax.dot_general(high, table_low[...], dims, preferred_element_type=F32)
    correction = first[:flat] + first[flat:] + second

    lane = lax.broadcasted_iota(jnp.int32, (z.rows, LANES), 1)
    before = blocks[z.n - 1][pl.ds(z.planes, z.rows), :]
    after = blocks[1][pl.ds(z.planes, z.rows), :]
    for a in range(z.axial):
        lows = [column(before, HALF + v * z.axial + a) for v in span]
        highs = [column(after, v * z.axial + a) for v in span]
        for h in range(z.tiles):
            at = pl.ds(a * z.block + h * z.rows, z.rows)
            for i in span:
                value = source[i, at, :]
                if h == 0:
                    edge = total([lows[j] * scalar(2, i, j) for j in span])
                    value = value - jnp.where(lane == 0, edge, 0.0)
                if h == z.tiles - 1:
                    edge = total([highs[j] * scalar(3, i, j) for j in span])
                    value = value - jnp.where(lane == LANES - 1, edge, 0.0)
                for q, plane_a in enumerate((0, z.axial - 1)):
                    if a == plane_a:
                        first = (q * z.v + i) * z.rows
                        value = value + correction[
                            first : first + z.rows, h * LANES : (h + 1) * LANES
                        ]
                total_source[i, at, :] = value

    stars = []
    for r in range(z.rows):
        row = [total_source[j, pl.ds(r, z.cells, stride=z.rows), :] for j in span]
        new = matvec(lambda i, j: ops[r, 2 * vv + i * z.v + j], row)
        for i in span:
            driven[r, i] = new[i]
        if r:
            new = plus(new, matvec(lambda i, j: ops[r, i * z.v + j], stars[-1]))
        stars.append(new)
    back = stars[-1]
    for r in range(z.rows - 2, -1, -1):
        back = plus(stars[r], matvec(lambda i, j: ops[r, vv + i * z.v + j], back))
    for i in span:
        vectors[i] = stars[-1][i]
        vectors[z.v + i] = back[i]


def place_pair(where, own, other, slots, lower, upper):
    def fill(a, b):
        for k, m in enumerate(lower):
            slots[k] = a[m]
        for k, m in enumerate(upper):
            slots[len(lower) + k] = b[m]

    @pl.when(where == 0)
    def _():
        fill(own, other)

    @pl.when(where != 0)
    def _():
        fill(other, own)


def merge_maps_kernel(z, level, device, own, other, out, slots):
    vv = z.vv
    every = list(range(3 * vv))
    place_pair((device[0] >> level) & 1, own, other, slots, every, every)
    span = range(z.v)

    def column(base, k):
        return [slots[base + j * z.v + k] for j in span]

    def apply(base, vector):
        return matvec(lambda i, j: slots[base + i * z.v + j], vector)

    up = 3 * vv
    for k in span:
        state = column(0, k)
        back = plus(column(vv, k), apply(2 * vv, apply(up + vv, state)))
        state = apply(up, state)
        through = apply(2 * vv, column(up + 2 * vv, k))
        for i in span:
            out[i * z.v + k] = state[i]
            out[vv + i * z.v + k] = back[i]
            out[2 * vv + i * z.v + k] = through[i]


def merge_response_kernel(z, level, device, own, other, out, slots):
    vv = z.vv
    place_pair((device[0] >> level) & 1, own, other, slots, range(3 * vv), range(2 * vv))
    span = range(z.v)

    def apply(base, vector):
        return matvec(lambda i, j: slots[base + i * z.v + j], vector)

    for k in span:
        column = [slots[j * z.v + k] for j in span]
        column = apply(2 * vv, apply(4 * vv, column))
        for i in span:
            out[i * z.v + k] = slots[vv + i * z.v + k] + column[i]


def merge_last_kernel(z, level, device, *refs):
    own_maps, other_maps = refs[: z.parts], refs[z.parts : 2 * z.parts]
    own, other, out, state_out, slots, vectors = refs[2 * z.parts :]
    vv = z.vv
    span = range(z.v)
    bit = (device[0] >> level) & 1
    half = (device[0] >> (level + 1)) & 1
    every = list(range(2 * z.v))
    place_pair(bit, own, other, vectors, every, every)
    lower, upper = range(3 * vv), range(2 * vv)
    for part in range(z.parts):
        at = pl.ds(part * z.chunk, z.chunk)
        place_pair(bit, own_maps[part], other_maps[part], slots, lower, upper)

        def apply(base, vector):
            return matvec(lambda i, j: slots[base + i * z.v + j], vector)

        fa, ha, fb, hb = [[vectors[k * z.v + i, at, :] for i in span] for k in range(4)]
        state = plus(fb, apply(3 * vv, fa))
        back = plus(ha, apply(2 * vv, plus(hb, apply(4 * vv, fa))))
        for i in span:
            state_out[i, at, :] = state[i]
            out[part * z.v + i] = jnp.where(half == 0, state[i], back[i])
        if part + 1 < z.parts:
            continue
        for k in span:
            column = [slots[j * z.v + k] for j in span]
            column = apply(2 * vv, apply(4 * vv, column))
            for i in span:
                out[z.parts * z.v + i * z.v + k] = slots[vv + i * z.v + k] + column[i]


def merge_vectors_kernel(z, level, device, *refs):
    own_maps, other_maps = refs[: z.parts], refs[z.parts : 2 * z.parts]
    own, other, out, slots, vectors = refs[2 * z.parts :]
    vv = z.vv
    span = range(z.v)
    bit = (device[0] >> level) & 1
    every = list(range(2 * z.v))
    place_pair(bit, own, other, vectors, every, every)
    for part in range(z.parts):
        at = pl.ds(part * z.chunk, z.chunk)
        place_pair(
            bit, own_maps[part], other_maps[part], slots, range(2 * vv, 3 * vv), range(2 * vv)
        )

        def apply(base, vector):
            return matvec(lambda i, j: slots[base + i * z.v + j], vector)

        fa, ha, fb, hb = [[vectors[k * z.v + i, at, :] for i in span] for k in range(4)]
        state = plus(fb, apply(vv, fa))
        back = plus(ha, apply(0, plus(hb, apply(2 * vv, fa))))
        for i in span:
            out[i, at, :] = state[i]
            out[z.v + i, at, :] = back[i]


def final_kernel(z, levels, device, *refs):
    span = range(z.v)
    vv = z.vv
    refs = list(refs)

    def take(count):
        taken = refs[:count]
        del refs[:count]
        return taken

    inner_maps = [(take(z.parts), take(z.parts)) for _ in range(levels - 1)]
    vector_pairs = [take(2) for _ in range(levels - 1)]
    responses = take(z.parts - 1)
    own_state, told, ops, driven, out, slots, vectors, inside, stars = refs

    def load(base, at):
        return [inside[base + i, at, :] for i in span]

    half = (device[0] >> (levels - 1)) & 1
    for part in range(z.parts):
        at = pl.ds(part * z.chunk, z.chunk)
        word = [told[part * z.v + i] for i in span]
        g, base = (responses[part], 0) if part + 1 < z.parts else (told, z.parts * z.v)
        state = [own_state[i, at, :] for i in span]
        back = matvec(lambda i, j: g[base + i * z.v + j], state)
        for i in span:
            zero = jnp.zeros_like(word[i])
            inside[i, at, :] = jnp.where(half == 0, zero, word[i])
            inside[z.v + i, at, :] = jnp.where(half == 0, word[i] + back[i], zero)

    for level in range(levels - 2, -1, -1):
        bit = (device[0] >> level) & 1
        own, other = vector_pairs[level]
        place_pair(bit, own, other, vectors, range(z.v), range(z.v, 2 * z.v))
        for part in range(z.parts):
            at = pl.ds(part * z.chunk, z.chunk)
            fa, hb = [[vectors[k * z.v + i, at, :] for i in span] for k in range(2)]
            own, other = inner_maps[level]
            place_pair(bit, own[part], other[part], slots, range(vv), range(vv, 3 * vv))

            def apply(base, vector):
                return matvec(lambda i, j: slots[base + i * z.v + j], vector)

            xa, yb = load(0, at), load(z.v, at)
            xb = plus(fa, apply(0, xa))
            ya = plus(plus(hb, apply(vv, xb)), apply(2 * vv, yb))
            for i in span:
                inside[i, at, :] = jnp.where(bit == 0, xa[i], xb[i])
                inside[z.v + i, at, :] = jnp.where(bit == 0, ya[i], yb[i])

    x = [inside[i] for i in span]
    y = [inside[z.v + i] for i in span]
    for r in range(z.rows):
        x = plus([driven[r, i] for i in span], matvec(lambda i, j: ops[r, i * z.v + j], x))
        for i in span:
            stars[r, i] = x[i]
    for r in range(z.rows - 1, -1, -1):
        y = plus(
            [stars[r, i] for i in span], matvec(lambda i, j: ops[r, vv + i * z.v + j], y)
        )
        for i in span:
            out[i, pl.ds(r, z.cells, stride=z.rows), :] = y[i]


def trig_tables(z):
    q = np.arange(z.width)[:, None]
    k = (np.arange(z.n)[:, None] + z.n * np.arange(z.per)[None, :]).reshape(1, z.n, 1, z.per)
    angle = 2 * np.pi * ((q.reshape(-1, 1, 1, 1) * k) % z.points) / z.points
    values = np.concatenate([np.cos(angle), np.sin(angle)], axis=2).reshape(z.width, -1)
    high = values.astype(np.float32).astype(ml_dtypes.bfloat16)
    low = (values - high.astype(np.float64)).astype(np.float32).astype(ml_dtypes.bfloat16)
    return high, low


def exchange(value, span, level, mirrored=False):
    flip = (2 << level) - 2 if mirrored else 1 << level
    return lax.ppermute(value, "span", [(d ^ flip, d) for d in range(span)])


def body(residual, inverse_diagonal, prior_increment, coupling, characteristic, cutoffs):
    pitch, span = lax.axis_size("pitch"), lax.axis_size("span")
    z = Sizes(residual, characteristic, pitch)
    vv = z.vv
    levels = span.bit_length() - 1
    residual_t = to_tiles(residual, z)
    prior_t = to_tiles(prior_increment, z)
    diag_t = to_tiles(inverse_diagonal, z)
    couple = jnp.transpose(coupling, (1, 0, 2))
    char = jnp.transpose(characteristic, (0, 3, 4, 1, 2)).reshape(-1, 2, z.harmonics)
    device = lax.axis_index("span").astype(jnp.int32).reshape(1)
    cell, part_cell = (z.cells, LANES), (z.chunk, LANES)
    field = (z.v, z.axial * z.block, LANES)
    scratch = pltpu.VMEM

    high, low = [jnp.asarray(table) for table in trig_tables(z)]
    residual_t, prior_t, couple, payload, ops, *maps = call(
        functools.partial(opening_kernel, z),
        [field, field, couple.shape, (z.planes + z.rows, LANES), (z.rows, 3 * vv) + cell]
        + [(3 * vv,) + part_cell] * z.parts,
        (couple, diag_t, prior_t, residual_t, device),
        [HBM] * 4 + [SMEM],
        [
            scratch((3 * vv,) + cell, F32),
            scratch((z.rows, vv) + cell, F32),
            scratch(diag_t.shape, F32),
            scratch((2 * vv,) + cell, F32),
            pltpu.SemaphoreType.DMA((8,)),
        ],
        flops=10_000_000,
    )
    blocks = [payload]
    for j in range(1, pitch):
        pairs = [((e + j) % pitch, e) for e in range(pitch)]
        blocks.append(lax.ppermute(payload, "pitch", pairs))

    map_levels = []
    for level in range(levels - 1):
        others = []
        for value in maps:
            others.append(exchange(value, span, level))
        map_levels.append((maps, others))
        if level + 2 < levels:
            maps = [
                call(
                    functools.partial(merge_maps_kernel, z, level),
                    [(3 * vv,) + part_cell],
                    (device, mine, other),
                    [SMEM, VMEM, VMEM],
                    [scratch((6 * vv,) + part_cell, F32)],
                )[0]
                for mine, other in zip(maps, others)
            ]

    source, spec, splats, high, low = call(
        functools.partial(prepare_kernel, z),
        [
            field,
            (2, 2 * vv, z.harmonics),
            (2 * vv, z.rows, LANES),
            (high.shape, BF16),
            (low.shape, BF16),
        ],
        (prior_t, residual_t, couple, char, cutoffs.reshape(1, 2), high, low),
        [VMEM] * 3 + [HBM] * 4,
        [
            scratch(char.shape, F32),
            scratch((1, 2), jnp.int32),
            pltpu.SemaphoreType.DMA((4,)),
        ],
        flops=5_000_000,
    )

    rows = 2 * z.v * z.rows
    driven, vectors = call(
        functools.partial(spectral_kernel, z),
        [(z.rows, z.v) + cell, (2 * z.v,) + cell],
        (*blocks, high, low, spec, ops, source, splats),
        [VMEM] * (z.n + 6),
        [
            scratch((rows, z.harmonics), F32),
            scratch((rows, z.harmonics), F32),
            scratch(field, F32),
        ],
        flops=10_000_000,
    )

    vector_levels = []
    for level in range(levels - 1):
        other = exchange(vectors, span, level)
        vector_levels.append((vectors, other))
        mine, others = map_levels[level]
        ins = (device, *mine, *others, vectors, other)
        specs = [SMEM] + [VMEM] * (2 * z.parts + 2)
        if level + 2 < levels:
            vectors = call(
                functools.partial(merge_vectors_kernel, z, level),
                [(2 * z.v,) + cell],
                ins,
                specs,
                [scratch((3 * vv,) + part_cell, F32), scratch((4 * z.v,) + cell, F32)],
            )[0]
        else:
            tell, state = call(
                functools.partial(merge_last_kernel, z, level),
                [(z.parts * z.v + vv,) + part_cell, (z.v,) + cell],
                ins,
                specs,
                [scratch((5 * vv,) + part_cell, F32), scratch((4 * z.v,) + cell, F32)],
            )
    responses = []
    for part in range(z.parts - 1):
        given = [side[part] for side in map_levels[-1]]
        response = call(
            functools.partial(merge_response_kernel, z, levels - 2),
            [(vv,) + part_cell],
            (device, *given),
            [SMEM, VMEM, VMEM],
            [scratch((5 * vv,) + part_cell, F32)],
        )[0]
        responses.append(exchange(response, span, levels - 1, MIRRORED))
    told = exchange(tell, span, levels - 1, MIRRORED)

    arrays = []
    for mine, others in map_levels:
        arrays += [*mine, *others]
    for pair in vector_levels:
        arrays += pair
    arrays += [*responses, state, told]
    update = call(
        functools.partial(final_kernel, z, levels),
        [field],
        (device, *arrays, ops, driven),
        [SMEM] + [VMEM] * (len(arrays) + 2),
        [
            scratch((3 * vv,) + part_cell, F32),
            scratch((2 * z.v,) + cell, F32),
            scratch((2 * z.v,) + cell, F32),
            scratch((z.rows, z.v) + cell, F32),
        ],
        flops=2_000_000,
    )[0]
    return from_tiles(update, z)


def solution(mesh):
    in_specs = (
        P(None, None, "span", "pitch"),
        P(None, None, None, "span", "pitch"),
        P(None, None, "span", "pitch"),
        P(),
        P(),
        P(),
    )
    out_specs = P(None, None, "span", "pitch")
    return jax.shard_map(body, mesh=mesh, in_specs=in_specs, out_specs=out_specs, check_vma=False)
```

```python
import functools

import jax
import jax.numpy as jnp
import ml_dtypes
import numpy as np
from jax import lax
from jax.experimental import pallas as pl
from jax.experimental.pallas import tpu as pltpu
from jax.sharding import PartitionSpec as P


LANES = 128
HALF = 64
VMEM = pl.BlockSpec(memory_space=pltpu.VMEM)
SMEM = pl.BlockSpec(memory_space=pltpu.SMEM)
HBM = pl.BlockSpec(memory_space=pltpu.HBM)
ANY = pl.BlockSpec(memory_space=pl.ANY)
PARTS = 2
MIRRORED = False
F32 = jnp.float32
BF16 = jnp.bfloat16


def call(kernel, outs, ins, specs, scratch=(), flops=1_000_000):
    moved = 4 * sum(int(np.prod(a.shape)) for a in ins)
    ins = [
        pltpu.with_memory_space_constraint(a, pltpu.HBM) if spec is HBM else a
        for a, spec in zip(ins, specs)
    ]
    return kernel_call(kernel, outs, ins, specs, scratch, flops, moved)


def kernel_call(kernel, outs, ins, specs, scratch, flops, moved):
    return pl.pallas_call(
        kernel,
        out_shape=[
            jax.ShapeDtypeStruct(*s) if isinstance(s[0], tuple) else jax.ShapeDtypeStruct(s, F32)
            for s in outs
        ],
        in_specs=list(specs),
        out_specs=[VMEM] * len(outs),
        scratch_shapes=list(scratch),
        cost_estimate=pl.CostEstimate(flops=flops, bytes_accessed=moved, transcendentals=0),
        compiler_params=pltpu.CompilerParams(vmem_limit_bytes=12 * 1024 * 1024),
    )(*ins)


def total(terms):
    terms = list(terms)
    while len(terms) > 1:
        paired = [a + b for a, b in zip(terms[::2], terms[1::2])]
        terms = paired + terms[2 * len(paired) :]
    return terms[0]


def matvec(get, vector):
    size = len(vector)
    return [total([get(i, j) * vector[j] for j in range(size)]) for i in range(size)]


def plus(a, b):
    return [x + y for x, y in zip(a, b)]


def split(x):
    high = x.astype(BF16)
    return high, (x - high.astype(F32)).astype(BF16)


def splat(coupling, which, i, j, shape):
    return jnp.broadcast_to(coupling[i, which : which + 1, j : j + 1], shape)


class Sizes:
    def __init__(self, residual, characteristic, pitch):
        self.v, self.axial, self.rows, self.width = residual.shape
        self.tiles = self.width // LANES
        self.block = self.tiles * self.rows
        self.cells = self.axial * self.tiles
        self.n = pitch
        self.points = pitch * self.width
        self.harmonics = characteristic.shape[2]
        self.per = self.harmonics // pitch
        self.planes = 2 * self.v * self.block
        self.vv = self.v * self.v
        self.parts = PARTS
        self.chunk = self.cells // self.parts


def to_tiles(array, sizes):
    lead = array.shape[:-3]
    array = array.reshape(lead + (sizes.axial, sizes.rows, sizes.tiles, LANES))
    array = jnp.swapaxes(array, -3, -2)
    return array.reshape((-1, sizes.axial * sizes.block, LANES))


def from_tiles(array, sizes):
    array = array.reshape((sizes.v, sizes.axial, sizes.tiles, sizes.rows, LANES))
    array = jnp.swapaxes(array, -3, -2)
    return array.reshape((sizes.v, sizes.axial, sizes.rows, sizes.width))


def opening_kernel(z, *refs):
    ins, refs = refs[:8], refs[9:]
    residual, prior, coupling, char, cutoffs, high, low, payload, ops = refs[:9]
    outs, (maps, powers, diag, splats, sems) = refs[9 : 9 + z.parts], refs[9 + z.parts :]
    span = range(z.v)
    vv = z.vv
    coupling_h, diag_h, prior_h, residual_h = ins[:4]
    pairs = [(coupling_h, coupling), (prior_h, prior), (residual_h, residual)]
    for i in span:
        at = pl.ds(i * z.v, z.v)
        pairs.append((diag_h.at[at], diag.at[at]))
    pairs += list(zip(ins[4:], (char, cutoffs, high, low)))
    copies = [pltpu.make_async_copy(a, b, sems.at[k]) for k, (a, b) in enumerate(pairs)]
    for copy in copies:
        copy.start()

    copies[0].wait()
    for which in range(2):
        for i in span:
            for j in span:
                splats[which * vv + i * z.v + j] = -splat(
                    coupling, which, i, j, (z.cells, LANES)
                )
    copies[1].wait()
    lane = lax.broadcasted_iota(jnp.int32, (z.rows, LANES), 1)
    halo = jnp.zeros((z.rows, LANES), F32)
    for v in span:
        for a in range(z.axial):
            first = prior[v, pl.ds(a * z.block, z.rows), :][:, 0:1]
            last = prior[v, pl.ds((a + 1) * z.block - z.rows, z.rows), :][:, LANES - 1 :]
            halo = jnp.where(lane == v * z.axial + a, first, halo)
            halo = jnp.where(lane == HALF + v * z.axial + a, last, halo)
    payload[pl.ds(z.planes, z.rows), :] = halo
    copies[2].wait()
    for q, a in enumerate((0, z.axial - 1)):
        for v in span:
            payload[pl.ds((q * z.v + v) * z.block, z.block), :] = residual[
                v, pl.ds(a * z.block, z.block), :
            ]

    for i in span:
        copies[3 + i].wait()

        def operators(r, _, i=i):
            d = [diag[i * z.v + j, pl.ds(r, z.cells, stride=z.rows), :] for j in span]
            for k in span:
                for which in range(2):
                    ops[r, which * vv + i * z.v + k] = total(
                        [d[j] * splats[which * vv + j * z.v + k] for j in span]
                    )
                ops[r, 2 * vv + i * z.v + k] = d[k]
            return 0

        lax.fori_loop(0, z.rows, operators, 0, unroll=True)

    for m in range(vv):
        powers[0, m] = ops[0, m]

    def forward(r, _):
        for k in span:
            column = [powers[r - 1, j * z.v + k] for j in span]
            new = matvec(lambda i, j: ops[r, i * z.v + j], column)
            for i in span:
                powers[r, i * z.v + k] = new[i]
        return 0

    lax.fori_loop(1, z.rows, forward, 0, unroll=True)
    top = z.rows - 1
    for m in range(vv):
        maps[m] = powers[top, m]
        maps[vv + m] = powers[top, m]
        maps[2 * vv + m] = ops[top, vv + m]

    def backward(step, _):
        r = top - step
        for k in span:
            for base in (vv, 2 * vv):
                column = [maps[base + j * z.v + k] for j in span]
                new = matvec(lambda i, j: ops[r, vv + i * z.v + j], column)
                for i in span:
                    value = new[i]
                    if base == vv:
                        value = value + powers[r, i * z.v + k]
                    maps[base + i * z.v + k] = value
        return 0

    lax.fori_loop(1, z.rows, backward, 0, unroll=True)
    for part in range(z.parts):
        for m in range(3 * vv):
            outs[part][m] = maps[m, pl.ds(part * z.chunk, z.chunk), :]
    for copy in copies[3 + z.v :]:
        copy.wait()


def prepare_kernel(z, prior, residual, coupling, char, cutoffs, source, spec, splats):
    span = range(z.v)
    vv = z.vv
    shape = (z.rows, LANES)
    factors = {
        (which, i, j): splat(coupling, which, i, j, shape)
        for which in range(2, 6)
        for i in span
        for j in span
    }
    for which in range(2, 4):
        for i in span:
            for j in span:
                splats[(which - 2) * vv + i * z.v + j] = factors[which, i, j]

    def scalar(which, i, j):
        return factors[which, i, j]

    lane = lax.broadcasted_iota(jnp.int32, (z.rows, LANES), 1)

    def tile(ref, v, a, h):
        return ref[v, pl.ds(a * z.block + h * z.rows, z.rows), :]

    for a in range(z.axial):
        here = [[tile(prior, v, a, h) for h in range(z.tiles)] for v in span]
        up = [[pltpu.roll(x, 1, 1) for x in row] for row in here]
        down = [[pltpu.roll(x, LANES - 1, 1) for x in row] for row in here]
        for h in range(z.tiles):
            lower, upper = [], []
            for v in span:
                edge = up[v][h - 1] if h else jnp.zeros((z.rows, LANES), F32)
                lower.append(jnp.where(lane == 0, edge, up[v][h]))
                edge = down[v][h + 1] if h + 1 < z.tiles else jnp.zeros((z.rows, LANES), F32)
                upper.append(jnp.where(lane == LANES - 1, edge, down[v][h]))
            terms = [(2, lower), (3, upper)]
            if a > 0:
                terms.append((4, [tile(prior, v, a - 1, h) for v in span]))
            if a + 1 < z.axial:
                terms.append((5, [tile(prior, v, a + 1, h) for v in span]))
            for i in span:
                value = tile(residual, i, a, h)
                for which, field in terms:
                    value = value - total([field[j] * scalar(which, i, j) for j in span])
                source[i, pl.ds(a * z.block + h * z.rows, z.rows), :] = value

    place = lax.broadcasted_iota(jnp.int32, (1, z.harmonics), 1)
    harmonic = (place % z.per) * z.n + place // z.per
    k_of = lax.broadcasted_iota(jnp.int32, (z.harmonics, z.harmonics), 0)
    select = jnp.where(k_of == harmonic, 1.0, 0.0).astype(BF16)
    value = jnp.concatenate([char[:, c, :] for c in range(2)], axis=0)
    high = value.astype(BF16)
    middle, low = split(value - high.astype(F32))
    ordered = total(
        [jnp.dot(part, select, preferred_element_type=F32) for part in (high, middle, low)]
    )
    weight = jnp.where(harmonic == 0, 1.0, 2.0) / z.points
    for q in range(2):
        factor = jnp.where(harmonic < cutoffs[:, q : q + 1], weight, 0.0)
        for c in range(2):
            first = (2 * c + q) * vv
            spec[c, pl.ds(q * vv, vv), :] = ordered[first : first + vv] * factor


def spectral_kernel(z, *refs):
    blocks = refs[: z.n]
    table_high, table_low, spec, ops, source, splats, driven, vectors, real, imag, total_source = (
        refs[z.n :]
    )
    span = range(z.v)
    vv = z.vv
    flat = 2 * z.v * z.rows

    def scalar(which, i, j):
        return splats[(which - 2) * vv + i * z.v + j]

    def column(halo, at):
        return jnp.broadcast_to(halo[:, at : at + 1], (z.rows, LANES))

    def plane(ref):
        value = ref[pl.ds(0, z.planes), :].reshape(2 * z.v, z.tiles, z.rows, LANES)
        parts = [value[:, h].reshape(flat, LANES) for h in range(z.tiles)]
        return parts[0] if len(parts) == 1 else jnp.concatenate(parts, axis=1)

    x = [plane(ref) for ref in blocks]

    def combine(coefficients):
        terms = []
        for c, value in zip(coefficients, x):
            if abs(c) < 1e-12:
                continue
            if abs(c - 1) < 1e-12:
                terms.append(value)
            elif abs(c + 1) < 1e-12:
                terms.append(-value)
            else:
                terms.append(value * float(c))
        return total(terms) if terms else None

    def table(ref, s):
        return ref[:, pl.ds(2 * z.per * s, 2 * z.per)]

    turns = 2 * np.pi * np.arange(z.n) / z.n
    for s in range(z.n // 2 + 1):
        yr = combine(np.cos(turns * s))
        yi = combine(-np.sin(turns * s))
        highs, lows = zip(*[split(y) for y in (yr, yi) if y is not None])
        both = jnp.concatenate(highs + lows, axis=0)
        high = jnp.concatenate(highs, axis=0) if len(highs) > 1 else highs[0]
        rows = high.shape[0]
        for t in sorted({s, (z.n - s) % z.n}):
            first = jnp.dot(both, table(table_high, t), preferred_element_type=F32)
            second = jnp.dot(high, table(table_low, t), preferred_element_type=F32)
            y = first[:rows] + first[rows:] + second
            re, im = y[:flat, : z.per], -y[:flat, z.per :]
            if yi is not None:
                sign = 1.0 if t == s else -1.0
                re = re + sign * y[flat:, z.per :]
                im = im + sign * y[flat:, : z.per]
            real[:, pl.ds(z.per * t, z.per)] = re
            imag[:, pl.ds(z.per * t, z.per)] = im

    out_real, out_imag = [], []
    for q in range(2):
        rows = [pl.ds((q * z.v + j) * z.rows, z.rows) for j in span]
        re = [real[at, :] for at in rows]
        im = [imag[at, :] for at in rows]
        for i in span:
            base = (q * z.v + i) * z.v
            cr = [spec[0, pl.ds(base + j, 1), :] for j in span]
            ci = [spec[1, pl.ds(base + j, 1), :] for j in span]
            out_real.append(total([cr[j] * re[j] - ci[j] * im[j] for j in span]))
            out_imag.append(total([cr[j] * im[j] + ci[j] * re[j] for j in span]))
    cr = jnp.concatenate(out_real, axis=0)
    ci = -jnp.concatenate(out_imag, axis=0)
    parts = []
    for s in range(z.n):
        at = slice(s * z.per, (s + 1) * z.per)
        parts += [cr[:, at], ci[:, at]]
    high, low = split(jnp.concatenate(parts, axis=1))
    dims = (((1,), (1,)), ((), ()))
    both = jnp.concatenate([high, low], axis=0)
    first = lax.dot_general(both, table_high[...], dims, preferred_element_type=F32)
    second = lax.dot_general(high, table_low[...], dims, preferred_element_type=F32)
    correction = first[:flat] + first[flat:] + second

    lane = lax.broadcasted_iota(jnp.int32, (z.rows, LANES), 1)
    before = blocks[z.n - 1][pl.ds(z.planes, z.rows), :]
    after = blocks[1][pl.ds(z.planes, z.rows), :]
    for a in range(z.axial):
        lows = [column(before, HALF + v * z.axial + a) for v in span]
        highs = [column(after, v * z.axial + a) for v in span]
        for h in range(z.tiles):
            at = pl.ds(a * z.block + h * z.rows, z.rows)
            for i in span:
                value = source[i, at, :]
                if h == 0:
                    edge = total([lows[j] * scalar(2, i, j) for j in span])
                    value = value - jnp.where(lane == 0, edge, 0.0)
                if h == z.tiles - 1:
                    edge = total([highs[j] * scalar(3, i, j) for j in span])
                    value = value - jnp.where(lane == LANES - 1, edge, 0.0)
                for q, plane_a in enumerate((0, z.axial - 1)):
                    if a == plane_a:
                        first = (q * z.v + i) * z.rows
                        value = value + correction[
                            first : first + z.rows, h * LANES : (h + 1) * LANES
                        ]
                total_source[i, at, :] = value

    stars = []
    for r in range(z.rows):
        row = [total_source[j, pl.ds(r, z.cells, stride=z.rows), :] for j in span]
        new = matvec(lambda i, j: ops[r, 2 * vv + i * z.v + j], row)
        for i in span:
            driven[r, i] = new[i]
        if r:
            new = plus(new, matvec(lambda i, j: ops[r, i * z.v + j], stars[-1]))
        stars.append(new)
    back = stars[-1]
    for r in range(z.rows - 2, -1, -1):
        back = plus(stars[r], matvec(lambda i, j: ops[r, vv + i * z.v + j], back))
    for i in span:
        vectors[i] = stars[-1][i]
        vectors[z.v + i] = back[i]


def place_pair(where, own, other, slots, lower, upper):
    def fill(a, b):
        for k, m in enumerate(lower):
            slots[k] = a[m]
        for k, m in enumerate(upper):
            slots[len(lower) + k] = b[m]

    @pl.when(where == 0)
    def _():
        fill(own, other)

    @pl.when(where != 0)
    def _():
        fill(other, own)


def merge_maps_kernel(z, level, device, own, other, out, slots):
    vv = z.vv
    every = list(range(3 * vv))
    place_pair((device[0] >> level) & 1, own, other, slots, every, every)
    span = range(z.v)

    def column(base, k):
        return [slots[base + j * z.v + k] for j in span]

    def apply(base, vector):
        return matvec(lambda i, j: slots[base + i * z.v + j], vector)

    up = 3 * vv
    for k in span:
        state = column(0, k)
        back = plus(column(vv, k), apply(2 * vv, apply(up + vv, state)))
        state = apply(up, state)
        through = apply(2 * vv, column(up + 2 * vv, k))
        for i in span:
            out[i * z.v + k] = state[i]
            out[vv + i * z.v + k] = back[i]
            out[2 * vv + i * z.v + k] = through[i]


def merge_response_kernel(z, level, device, own, other, out, slots):
    vv = z.vv
    place_pair((device[0] >> level) & 1, own, other, slots, range(3 * vv), range(2 * vv))
    span = range(z.v)

    def apply(base, vector):
        return matvec(lambda i, j: slots[base + i * z.v + j], vector)

    for k in span:
        column = [slots[j * z.v + k] for j in span]
        column = apply(2 * vv, apply(4 * vv, column))
        for i in span:
            out[i * z.v + k] = slots[vv + i * z.v + k] + column[i]


def merge_last_kernel(z, level, device, *refs):
    own_maps, other_maps = refs[: z.parts], refs[z.parts : 2 * z.parts]
    own, other, out, state_out, slots, vectors = refs[2 * z.parts :]
    vv = z.vv
    span = range(z.v)
    bit = (device[0] >> level) & 1
    half = (device[0] >> (level + 1)) & 1
    every = list(range(2 * z.v))
    place_pair(bit, own, other, vectors, every, every)
    lower, upper = range(3 * vv), range(2 * vv)
    for part in range(z.parts):
        at = pl.ds(part * z.chunk, z.chunk)
        place_pair(bit, own_maps[part], other_maps[part], slots, lower, upper)

        def apply(base, vector):
            return matvec(lambda i, j: slots[base + i * z.v + j], vector)

        fa, ha, fb, hb = [[vectors[k * z.v + i, at, :] for i in span] for k in range(4)]
        state = plus(fb, apply(3 * vv, fa))
        back = plus(ha, apply(2 * vv, plus(hb, apply(4 * vv, fa))))
        for i in span:
            state_out[i, at, :] = state[i]
            out[part * z.v + i] = jnp.where(half == 0, state[i], back[i])
        if part + 1 < z.parts:
            continue
        for k in span:
            column = [slots[j * z.v + k] for j in span]
            column = apply(2 * vv, apply(4 * vv, column))
            for i in span:
                out[z.parts * z.v + i * z.v + k] = slots[vv + i * z.v + k] + column[i]


def merge_vectors_kernel(z, level, device, *refs):
    own_maps, other_maps = refs[: z.parts], refs[z.parts : 2 * z.parts]
    own, other, out, slots, vectors = refs[2 * z.parts :]
    vv = z.vv
    span = range(z.v)
    bit = (device[0] >> level) & 1
    every = list(range(2 * z.v))
    place_pair(bit, own, other, vectors, every, every)
    for part in range(z.parts):
        at = pl.ds(part * z.chunk, z.chunk)
        place_pair(
            bit, own_maps[part], other_maps[part], slots, range(2 * vv, 3 * vv), range(2 * vv)
        )

        def apply(base, vector):
            return matvec(lambda i, j: slots[base + i * z.v + j], vector)

        fa, ha, fb, hb = [[vectors[k * z.v + i, at, :] for i in span] for k in range(4)]
        state = plus(fb, apply(vv, fa))
        back = plus(ha, apply(0, plus(hb, apply(2 * vv, fa))))
        for i in span:
            out[i, at, :] = state[i]
            out[z.v + i, at, :] = back[i]


def final_kernel(z, levels, device, *refs):
    span = range(z.v)
    vv = z.vv
    refs = list(refs)

    def take(count):
        taken = refs[:count]
        del refs[:count]
        return taken

    inner_maps = [(take(z.parts), take(z.parts)) for _ in range(levels - 1)]
    vector_pairs = [take(2) for _ in range(levels - 1)]
    responses = take(z.parts - 1)
    own_state, told, ops, driven, out, slots, vectors, inside, stars = refs

    def load(base, at):
        return [inside[base + i, at, :] for i in span]

    half = (device[0] >> (levels - 1)) & 1
    for part in range(z.parts):
        at = pl.ds(part * z.chunk, z.chunk)
        word = [told[part * z.v + i] for i in span]
        g, base = (responses[part], 0) if part + 1 < z.parts else (told, z.parts * z.v)
        state = [own_state[i, at, :] for i in span]
        back = matvec(lambda i, j: g[base + i * z.v + j], state)
        for i in span:
            zero = jnp.zeros_like(word[i])
            inside[i, at, :] = jnp.where(half == 0, zero, word[i])
            inside[z.v + i, at, :] = jnp.where(half == 0, word[i] + back[i], zero)

    for level in range(levels - 2, -1, -1):
        bit = (device[0] >> level) & 1
        own, other = vector_pairs[level]
        place_pair(bit, own, other, vectors, range(z.v), range(z.v, 2 * z.v))
        for part in range(z.parts):
            at = pl.ds(part * z.chunk, z.chunk)
            fa, hb = [[vectors[k * z.v + i, at, :] for i in span] for k in range(2)]
            own, other = inner_maps[level]
            place_pair(bit, own[part], other[part], slots, range(vv), range(vv, 3 * vv))

            def apply(base, vector):
                return matvec(lambda i, j: slots[base + i * z.v + j], vector)

            xa, yb = load(0, at), load(z.v, at)
            xb = plus(fa, apply(0, xa))
            ya = plus(plus(hb, apply(vv, xb)), apply(2 * vv, yb))
            for i in span:
                inside[i, at, :] = jnp.where(bit == 0, xa[i], xb[i])
                inside[z.v + i, at, :] = jnp.where(bit == 0, ya[i], yb[i])

    x = [inside[i] for i in span]
    y = [inside[z.v + i] for i in span]
    for r in range(z.rows):
        x = plus([driven[r, i] for i in span], matvec(lambda i, j: ops[r, i * z.v + j], x))
        for i in span:
            stars[r, i] = x[i]
    for r in range(z.rows - 1, -1, -1):
        y = plus(
            [stars[r, i] for i in span], matvec(lambda i, j: ops[r, vv + i * z.v + j], y)
        )
        for i in span:
            out[i, pl.ds(r, z.cells, stride=z.rows), :] = y[i]


def trig_tables(z):
    q = np.arange(z.width)[:, None]
    k = (np.arange(z.n)[:, None] + z.n * np.arange(z.per)[None, :]).reshape(1, z.n, 1, z.per)
    angle = 2 * np.pi * ((q.reshape(-1, 1, 1, 1) * k) % z.points) / z.points
    values = np.concatenate([np.cos(angle), np.sin(angle)], axis=2).reshape(z.width, -1)
    high = values.astype(np.float32).astype(ml_dtypes.bfloat16)
    low = (values - high.astype(np.float64)).astype(np.float32).astype(ml_dtypes.bfloat16)
    return high, low


def exchange(value, span, level, mirrored=False):
    flip = (2 << level) - 2 if mirrored else 1 << level
    return lax.ppermute(value, "span", [(d ^ flip, d) for d in range(span)])


def body(residual, inverse_diagonal, prior_increment, coupling, characteristic, cutoffs):
    pitch, span = lax.axis_size("pitch"), lax.axis_size("span")
    z = Sizes(residual, characteristic, pitch)
    vv = z.vv
    levels = span.bit_length() - 1
    residual_t = to_tiles(residual, z)
    prior_t = to_tiles(prior_increment, z)
    diag_t = to_tiles(inverse_diagonal, z)
    couple = jnp.transpose(coupling, (1, 0, 2))
    char = jnp.transpose(characteristic, (0, 3, 4, 1, 2)).reshape(-1, 2, z.harmonics)
    device = lax.axis_index("span").astype(jnp.int32).reshape(1)
    cell, part_cell = (z.cells, LANES), (z.chunk, LANES)
    field = (z.v, z.axial * z.block, LANES)
    scratch = pltpu.VMEM

    high, low = [jnp.asarray(table) for table in trig_tables(z)]
    cuts = cutoffs.reshape(1, 2)
    kept = [(char.shape, F32), (cuts.shape, jnp.int32), (high.shape, BF16), (low.shape, BF16)]
    ins = (couple, diag_t, prior_t, residual_t, char, cuts, high, low, device)
    residual_t, prior_t, couple, char, cuts, high, low, payload, ops, *maps = call(
        functools.partial(opening_kernel, z),
        [field, field, couple.shape, *kept, (z.planes + z.rows, LANES), (z.rows, 3 * vv) + cell]
        + [(3 * vv,) + part_cell] * z.parts,
        ins,
        [HBM] * 8 + [SMEM],
        [
            scratch((3 * vv,) + cell, F32),
            scratch((z.rows, vv) + cell, F32),
            scratch(diag_t.shape, F32),
            scratch((2 * vv,) + cell, F32),
            pltpu.SemaphoreType.DMA((z.v + 7,)),
        ],
        flops=10_000_000,
    )
    blocks = [payload]
    for j in range(1, pitch):
        pairs = [((e + j) % pitch, e) for e in range(pitch)]
        blocks.append(lax.ppermute(payload, "pitch", pairs))

    map_levels = []
    for level in range(levels - 1):
        others = []
        for value in maps:
            others.append(exchange(value, span, level))
        map_levels.append((maps, others))
        if level + 2 < levels:
            maps = [
                call(
                    functools.partial(merge_maps_kernel, z, level),
                    [(3 * vv,) + part_cell],
                    (device, mine, other),
                    [SMEM, VMEM, VMEM],
                    [scratch((6 * vv,) + part_cell, F32)],
                )[0]
                for mine, other in zip(maps, others)
            ]

    source, spec, splats = call(
        functools.partial(prepare_kernel, z),
        [field, (2, 2 * vv, z.harmonics), (2 * vv, z.rows, LANES)],
        (prior_t, residual_t, couple, char, cuts),
        [VMEM] * 5,
        flops=5_000_000,
    )

    rows = 2 * z.v * z.rows
    driven, vectors = call(
        functools.partial(spectral_kernel, z),
        [(z.rows, z.v) + cell, (2 * z.v,) + cell],
        (*blocks, high, low, spec, ops, source, splats),
        [VMEM] * (z.n + 6),
        [
            scratch((rows, z.harmonics), F32),
            scratch((rows, z.harmonics), F32),
            scratch(field, F32),
        ],
        flops=10_000_000,
    )

    vector_levels = []
    for level in range(levels - 1):
        other = exchange(vectors, span, level)
        vector_levels.append((vectors, other))
        mine, others = map_levels[level]
        ins = (device, *mine, *others, vectors, other)
        specs = [SMEM] + [VMEM] * (2 * z.parts + 2)
        if level + 2 < levels:
            vectors = call(
                functools.partial(merge_vectors_kernel, z, level),
                [(2 * z.v,) + cell],
                ins,
                specs,
                [scratch((3 * vv,) + part_cell, F32), scratch((4 * z.v,) + cell, F32)],
            )[0]
        else:
            tell, state = call(
                functools.partial(merge_last_kernel, z, level),
                [(z.parts * z.v + vv,) + part_cell, (z.v,) + cell],
                ins,
                specs,
                [scratch((5 * vv,) + part_cell, F32), scratch((4 * z.v,) + cell, F32)],
            )
    responses = []
    for part in range(z.parts - 1):
        given = [side[part] for side in map_levels[-1]]
        response = call(
            functools.partial(merge_response_kernel, z, levels - 2),
            [(vv,) + part_cell],
            (device, *given),
            [SMEM, VMEM, VMEM],
            [scratch((5 * vv,) + part_cell, F32)],
        )[0]
        responses.append(exchange(response, span, levels - 1, MIRRORED))
    told = exchange(tell, span, levels - 1, MIRRORED)

    arrays = []
    for mine, others in map_levels:
        arrays += [*mine, *others]
    for pair in vector_levels:
        arrays += pair
    arrays += [*responses, state, told]
    update = call(
        functools.partial(final_kernel, z, levels),
        [field],
        (device, *arrays, ops, driven),
        [SMEM] + [VMEM] * (len(arrays) + 2),
        [
            scratch((3 * vv,) + part_cell, F32),
            scratch((2 * z.v,) + cell, F32),
            scratch((2 * z.v,) + cell, F32),
            scratch((z.rows, z.v) + cell, F32),
        ],
        flops=2_000_000,
    )[0]
    return from_tiles(update, z)


def solution(mesh):
    in_specs = (
        P(None, None, "span", "pitch"),
        P(None, None, None, "span", "pitch"),
        P(None, None, "span", "pitch"),
        P(),
        P(),
        P(),
    )
    out_specs = P(None, None, "span", "pitch")
    return jax.shard_map(body, mesh=mesh, in_specs=in_specs, out_specs=out_specs, check_vma=False)
```

```python
import functools

import jax
import jax.numpy as jnp
import ml_dtypes
import numpy as np
from jax import lax
from jax.experimental import pallas as pl
from jax.experimental.pallas import tpu as pltpu
from jax.sharding import PartitionSpec as P


LANES = 128
HALF = 64
VMEM = pl.BlockSpec(memory_space=pltpu.VMEM)
SMEM = pl.BlockSpec(memory_space=pltpu.SMEM)
HBM = pl.BlockSpec(memory_space=pltpu.HBM)
ANY = pl.BlockSpec(memory_space=pl.ANY)
PARTS = 2
MIRRORED = False
F32 = jnp.float32
BF16 = jnp.bfloat16


def call(kernel, outs, ins, specs, scratch=(), flops=1_000_000):
    moved = 4 * sum(int(np.prod(a.shape)) for a in ins)
    ins = [
        pltpu.with_memory_space_constraint(a, pltpu.HBM) if spec is HBM else a
        for a, spec in zip(ins, specs)
    ]
    return kernel_call(kernel, outs, ins, specs, scratch, flops, moved)


def kernel_call(kernel, outs, ins, specs, scratch, flops, moved):
    return pl.pallas_call(
        kernel,
        out_shape=[
            jax.ShapeDtypeStruct(*s) if isinstance(s[0], tuple) else jax.ShapeDtypeStruct(s, F32)
            for s in outs
        ],
        in_specs=list(specs),
        out_specs=[VMEM] * len(outs),
        scratch_shapes=list(scratch),
        cost_estimate=pl.CostEstimate(flops=flops, bytes_accessed=moved, transcendentals=0),
        compiler_params=pltpu.CompilerParams(vmem_limit_bytes=12 * 1024 * 1024),
    )(*ins)


def total(terms):
    terms = list(terms)
    while len(terms) > 1:
        paired = [a + b for a, b in zip(terms[::2], terms[1::2])]
        terms = paired + terms[2 * len(paired) :]
    return terms[0]


def matvec(get, vector):
    size = len(vector)
    return [total([get(i, j) * vector[j] for j in range(size)]) for i in range(size)]


def plus(a, b):
    return [x + y for x, y in zip(a, b)]


def split(x):
    high = x.astype(BF16)
    return high, (x - high.astype(F32)).astype(BF16)


def splat(coupling, which, i, j, shape):
    return jnp.broadcast_to(coupling[i, which : which + 1, j : j + 1], shape)


class Sizes:
    def __init__(self, residual, characteristic, pitch):
        self.v, self.axial, self.rows, self.width = residual.shape
        self.tiles = self.width // LANES
        self.block = self.tiles * self.rows
        self.cells = self.axial * self.tiles
        self.n = pitch
        self.points = pitch * self.width
        self.harmonics = characteristic.shape[2]
        self.per = self.harmonics // pitch
        self.planes = 2 * self.v * self.block
        self.vv = self.v * self.v
        self.parts = PARTS
        self.chunk = self.cells // self.parts


def to_tiles(array, sizes):
    lead = array.shape[:-3]
    array = array.reshape(lead + (sizes.axial, sizes.rows, sizes.tiles, LANES))
    array = jnp.swapaxes(array, -3, -2)
    return array.reshape((-1, sizes.axial * sizes.block, LANES))


def from_tiles(array, sizes):
    array = array.reshape((sizes.v, sizes.axial, sizes.tiles, sizes.rows, LANES))
    array = jnp.swapaxes(array, -3, -2)
    return array.reshape((sizes.v, sizes.axial, sizes.rows, sizes.width))


def opening_kernel(z, *refs):
    ins, refs = refs[:8], refs[9:]
    residual, prior, coupling, char, cutoffs, high, low, payload, ops = refs[:9]
    outs, (maps, powers, diag, splats, sems) = refs[9 : 9 + z.parts], refs[9 + z.parts :]
    span = range(z.v)
    vv = z.vv
    coupling_h, diag_h, prior_h, residual_h = ins[:4]
    pairs = [(coupling_h, coupling), (prior_h, prior), (residual_h, residual)]
    for i in span:
        at = pl.ds(i * z.v, z.v)
        pairs.append((diag_h.at[at], diag.at[at]))
    pairs += list(zip(ins[4:], (char, cutoffs, high, low)))
    copies = [pltpu.make_async_copy(a, b, sems.at[k]) for k, (a, b) in enumerate(pairs)]
    for copy in copies:
        copy.start()

    copies[0].wait()
    for which in range(2):
        for i in span:
            for j in span:
                splats[which * vv + i * z.v + j] = -splat(
                    coupling, which, i, j, (z.cells, LANES)
                )
    copies[1].wait()
    lane = lax.broadcasted_iota(jnp.int32, (z.rows, LANES), 1)
    halo = jnp.zeros((z.rows, LANES), F32)
    for v in span:
        for a in range(z.axial):
            first = prior[v, pl.ds(a * z.block, z.rows), :][:, 0:1]
            last = prior[v, pl.ds((a + 1) * z.block - z.rows, z.rows), :][:, LANES - 1 :]
            halo = jnp.where(lane == v * z.axial + a, first, halo)
            halo = jnp.where(lane == HALF + v * z.axial + a, last, halo)
    payload[pl.ds(z.planes, z.rows), :] = halo
    copies[2].wait()
    for q, a in enumerate((0, z.axial - 1)):
        for v in span:
            payload[pl.ds((q * z.v + v) * z.block, z.block), :] = residual[
                v, pl.ds(a * z.block, z.block), :
            ]

    for i in span:
        copies[3 + i].wait()

        def operators(r, _, i=i):
            d = [diag[i * z.v + j, pl.ds(r, z.cells, stride=z.rows), :] for j in span]
            for k in span:
                for which in range(2):
                    ops[r, which * vv + i * z.v + k] = total(
                        [d[j] * splats[which * vv + j * z.v + k] for j in span]
                    )
                ops[r, 2 * vv + i * z.v + k] = d[k]
            return 0

        lax.fori_loop(0, z.rows, operators, 0, unroll=True)

    for m in range(vv):
        powers[0, m] = ops[0, m]

    def forward(r, _):
        for k in span:
            column = [powers[r - 1, j * z.v + k] for j in span]
            new = matvec(lambda i, j: ops[r, i * z.v + j], column)
            for i in span:
                powers[r, i * z.v + k] = new[i]
        return 0

    lax.fori_loop(1, z.rows, forward, 0, unroll=True)
    top = z.rows - 1
    for m in range(vv):
        maps[m] = powers[top, m]
        maps[vv + m] = powers[top, m]
        maps[2 * vv + m] = ops[top, vv + m]

    def backward(step, _):
        r = top - step
        for k in span:
            for base in (vv, 2 * vv):
                column = [maps[base + j * z.v + k] for j in span]
                new = matvec(lambda i, j: ops[r, vv + i * z.v + j], column)
                for i in span:
                    value = new[i]
                    if base == vv:
                        value = value + powers[r, i * z.v + k]
                    maps[base + i * z.v + k] = value
        return 0

    lax.fori_loop(1, z.rows, backward, 0, unroll=True)
    for part in range(z.parts):
        for m in range(3 * vv):
            outs[part][m] = maps[m, pl.ds(part * z.chunk, z.chunk), :]
    for copy in copies[3 + z.v :]:
        copy.wait()


def prepare_kernel(z, prior, residual, coupling, char, cutoffs, source, spec, splats):
    span = range(z.v)
    vv = z.vv
    shape = (z.rows, LANES)
    factors = {
        (which, i, j): splat(coupling, which, i, j, shape)
        for which in range(2, 6)
        for i in span
        for j in span
    }
    for which in range(2, 4):
        for i in span:
            for j in span:
                splats[(which - 2) * vv + i * z.v + j] = factors[which, i, j]

    def scalar(which, i, j):
        return factors[which, i, j]

    lane = lax.broadcasted_iota(jnp.int32, (z.rows, LANES), 1)

    def tile(ref, v, a, h):
        return ref[v, pl.ds(a * z.block + h * z.rows, z.rows), :]

    for a in range(z.axial):
        here = [[tile(prior, v, a, h) for h in range(z.tiles)] for v in span]
        up = [[pltpu.roll(x, 1, 1) for x in row] for row in here]
        down = [[pltpu.roll(x, LANES - 1, 1) for x in row] for row in here]
        for h in range(z.tiles):
            lower, upper = [], []
            for v in span:
                edge = up[v][h - 1] if h else jnp.zeros((z.rows, LANES), F32)
                lower.append(jnp.where(lane == 0, edge, up[v][h]))
                edge = down[v][h + 1] if h + 1 < z.tiles else jnp.zeros((z.rows, LANES), F32)
                upper.append(jnp.where(lane == LANES - 1, edge, down[v][h]))
            terms = [(2, lower), (3, upper)]
            if a > 0:
                terms.append((4, [tile(prior, v, a - 1, h) for v in span]))
            if a + 1 < z.axial:
                terms.append((5, [tile(prior, v, a + 1, h) for v in span]))
            for i in span:
                value = tile(residual, i, a, h)
                for which, field in terms:
                    value = value - total([field[j] * scalar(which, i, j) for j in span])
                source[i, pl.ds(a * z.block + h * z.rows, z.rows), :] = value

    place = lax.broadcasted_iota(jnp.int32, (1, z.harmonics), 1)
    harmonic = (place % z.per) * z.n + place // z.per
    k_of = lax.broadcasted_iota(jnp.int32, (z.harmonics, z.harmonics), 0)
    select = jnp.where(k_of == harmonic, 1.0, 0.0).astype(BF16)
    value = jnp.concatenate([char[:, c, :] for c in range(2)], axis=0)
    high = value.astype(BF16)
    middle, low = split(value - high.astype(F32))
    ordered = total(
        [jnp.dot(part, select, preferred_element_type=F32) for part in (high, middle, low)]
    )
    weight = jnp.where(harmonic == 0, 1.0, 2.0) / z.points
    for q in range(2):
        factor = jnp.where(harmonic < cutoffs[:, q : q + 1], weight, 0.0)
        for c in range(2):
            first = (2 * c + q) * vv
            spec[c, pl.ds(q * vv, vv), :] = ordered[first : first + vv] * factor


def spectral_kernel(z, *refs):
    blocks = refs[: z.n]
    table_high, table_low, spec, ops, source, splats, driven, vectors, real, imag, total_source = (
        refs[z.n :]
    )
    span = range(z.v)
    vv = z.vv
    flat = 2 * z.v * z.rows

    def scalar(which, i, j):
        return splats[(which - 2) * vv + i * z.v + j]

    def column(halo, at):
        return jnp.broadcast_to(halo[:, at : at + 1], (z.rows, LANES))

    def plane(ref):
        value = ref[pl.ds(0, z.planes), :].reshape(2 * z.v, z.tiles, z.rows, LANES)
        parts = [value[:, h].reshape(flat, LANES) for h in range(z.tiles)]
        return parts[0] if len(parts) == 1 else jnp.concatenate(parts, axis=1)

    x = [plane(ref) for ref in blocks]

    def combine(coefficients):
        terms = []
        for c, value in zip(coefficients, x):
            if abs(c) < 1e-12:
                continue
            if abs(c - 1) < 1e-12:
                terms.append(value)
            elif abs(c + 1) < 1e-12:
                terms.append(-value)
            else:
                terms.append(value * float(c))
        return total(terms) if terms else None

    def table(ref, s):
        return ref[:, pl.ds(2 * z.per * s, 2 * z.per)]

    turns = 2 * np.pi * np.arange(z.n) / z.n
    for s in range(z.n // 2 + 1):
        yr = combine(np.cos(turns * s))
        yi = combine(-np.sin(turns * s))
        highs, lows = zip(*[split(y) for y in (yr, yi) if y is not None])
        both = jnp.concatenate(highs + lows, axis=0)
        high = jnp.concatenate(highs, axis=0) if len(highs) > 1 else highs[0]
        rows = high.shape[0]
        for t in sorted({s, (z.n - s) % z.n}):
            first = jnp.dot(both, table(table_high, t), preferred_element_type=F32)
            second = jnp.dot(high, table(table_low, t), preferred_element_type=F32)
            y = first[:rows] + first[rows:] + second
            re, im = y[:flat, : z.per], -y[:flat, z.per :]
            if yi is not None:
                sign = 1.0 if t == s else -1.0
                re = re + sign * y[flat:, z.per :]
                im = im + sign * y[flat:, : z.per]
            real[:, pl.ds(z.per * t, z.per)] = re
            imag[:, pl.ds(z.per * t, z.per)] = im

    out_real, out_imag = [], []
    for q in range(2):
        rows = [pl.ds((q * z.v + j) * z.rows, z.rows) for j in span]
        re = [real[at, :] for at in rows]
        im = [imag[at, :] for at in rows]
        for i in span:
            base = (q * z.v + i) * z.v
            cr = [spec[0, pl.ds(base + j, 1), :] for j in span]
            ci = [spec[1, pl.ds(base + j, 1), :] for j in span]
            out_real.append(total([cr[j] * re[j] - ci[j] * im[j] for j in span]))
            out_imag.append(total([cr[j] * im[j] + ci[j] * re[j] for j in span]))
    cr = jnp.concatenate(out_real, axis=0)
    ci = -jnp.concatenate(out_imag, axis=0)
    parts = []
    for s in range(z.n):
        at = slice(s * z.per, (s + 1) * z.per)
        parts += [cr[:, at], ci[:, at]]
    high, low = split(jnp.concatenate(parts, axis=1))
    dims = (((1,), (1,)), ((), ()))
    both = jnp.concatenate([high, low], axis=0)
    first = lax.dot_general(both, table_high[...], dims, preferred_element_type=F32)
    second = lax.dot_general(high, table_low[...], dims, preferred_element_type=F32)
    correction = first[:flat] + first[flat:] + second

    lane = lax.broadcasted_iota(jnp.int32, (z.rows, LANES), 1)
    before = blocks[z.n - 1][pl.ds(z.planes, z.rows), :]
    after = blocks[1][pl.ds(z.planes, z.rows), :]
    for a in range(z.axial):
        lows = [column(before, HALF + v * z.axial + a) for v in span]
        highs = [column(after, v * z.axial + a) for v in span]
        for h in range(z.tiles):
            at = pl.ds(a * z.block + h * z.rows, z.rows)
            for i in span:
                value = source[i, at, :]
                if h == 0:
                    edge = total([lows[j] * scalar(2, i, j) for j in span])
                    value = value - jnp.where(lane == 0, edge, 0.0)
                if h == z.tiles - 1:
                    edge = total([highs[j] * scalar(3, i, j) for j in span])
                    value = value - jnp.where(lane == LANES - 1, edge, 0.0)
                for q, plane_a in enumerate((0, z.axial - 1)):
                    if a == plane_a:
                        first = (q * z.v + i) * z.rows
                        value = value + correction[
                            first : first + z.rows, h * LANES : (h + 1) * LANES
                        ]
                total_source[i, at, :] = value

    stars = []
    for r in range(z.rows):
        row = [total_source[j, pl.ds(r, z.cells, stride=z.rows), :] for j in span]
        new = matvec(lambda i, j: ops[r, 2 * vv + i * z.v + j], row)
        for i in span:
            driven[r, i] = new[i]
        if r:
            new = plus(new, matvec(lambda i, j: ops[r, i * z.v + j], stars[-1]))
        stars.append(new)
    back = stars[-1]
    for r in range(z.rows - 2, -1, -1):
        back = plus(stars[r], matvec(lambda i, j: ops[r, vv + i * z.v + j], back))
    for i in span:
        vectors[i] = stars[-1][i]
        vectors[z.v + i] = back[i]


def place_pair(where, own, other, slots, lower, upper):
    def fill(a, b):
        for k, m in enumerate(lower):
            slots[k] = a[m]
        for k, m in enumerate(upper):
            slots[len(lower) + k] = b[m]

    @pl.when(where == 0)
    def _():
        fill(own, other)

    @pl.when(where != 0)
    def _():
        fill(other, own)


def merge_maps_kernel(z, level, device, own, other, out, slots):
    vv = z.vv
    every = list(range(3 * vv))
    place_pair((device[0] >> level) & 1, own, other, slots, every, every)
    span = range(z.v)

    def column(base, k):
        return [slots[base + j * z.v + k] for j in span]

    def apply(base, vector):
        return matvec(lambda i, j: slots[base + i * z.v + j], vector)

    up = 3 * vv
    for k in span:
        state = column(0, k)
        back = plus(column(vv, k), apply(2 * vv, apply(up + vv, state)))
        state = apply(up, state)
        through = apply(2 * vv, column(up + 2 * vv, k))
        for i in span:
            out[i * z.v + k] = state[i]
            out[vv + i * z.v + k] = back[i]
            out[2 * vv + i * z.v + k] = through[i]


def merge_response_kernel(z, level, device, own, other, out, slots):
    vv = z.vv
    place_pair((device[0] >> level) & 1, own, other, slots, range(3 * vv), range(2 * vv))
    span = range(z.v)

    def apply(base, vector):
        return matvec(lambda i, j: slots[base + i * z.v + j], vector)

    for k in span:
        column = [slots[j * z.v + k] for j in span]
        column = apply(2 * vv, apply(4 * vv, column))
        for i in span:
            out[i * z.v + k] = slots[vv + i * z.v + k] + column[i]


def merge_last_kernel(z, level, device, *refs):
    own_maps, other_maps = refs[: z.parts], refs[z.parts : 2 * z.parts]
    own, other, out, state_out, slots, vectors = refs[2 * z.parts :]
    vv = z.vv
    span = range(z.v)
    bit = (device[0] >> level) & 1
    half = (device[0] >> (level + 1)) & 1
    every = list(range(2 * z.v))
    place_pair(bit, own, other, vectors, every, every)
    lower, upper = range(3 * vv), range(2 * vv)
    for part in range(z.parts):
        at = pl.ds(part * z.chunk, z.chunk)
        place_pair(bit, own_maps[part], other_maps[part], slots, lower, upper)

        def apply(base, vector):
            return matvec(lambda i, j: slots[base + i * z.v + j], vector)

        fa, ha, fb, hb = [[vectors[k * z.v + i, at, :] for i in span] for k in range(4)]
        state = plus(fb, apply(3 * vv, fa))
        back = plus(ha, apply(2 * vv, plus(hb, apply(4 * vv, fa))))
        for i in span:
            state_out[i, at, :] = state[i]
            out[part * z.v + i] = jnp.where(half == 0, state[i], back[i])
        if part + 1 < z.parts:
            continue
        for k in span:
            column = [slots[j * z.v + k] for j in span]
            column = apply(2 * vv, apply(4 * vv, column))
            for i in span:
                out[z.parts * z.v + i * z.v + k] = slots[vv + i * z.v + k] + column[i]


def merge_vectors_kernel(z, level, device, *refs):
    own_maps, other_maps = refs[: z.parts], refs[z.parts : 2 * z.parts]
    own, other, out, slots, vectors = refs[2 * z.parts :]
    vv = z.vv
    span = range(z.v)
    bit = (device[0] >> level) & 1
    every = list(range(2 * z.v))
    place_pair(bit, own, other, vectors, every, every)
    for part in range(z.parts):
        at = pl.ds(part * z.chunk, z.chunk)
        place_pair(
            bit, own_maps[part], other_maps[part], slots, range(2 * vv, 3 * vv), range(2 * vv)
        )

        def apply(base, vector):
            return matvec(lambda i, j: slots[base + i * z.v + j], vector)

        fa, ha, fb, hb = [[vectors[k * z.v + i, at, :] for i in span] for k in range(4)]
        state = plus(fb, apply(vv, fa))
        back = plus(ha, apply(0, plus(hb, apply(2 * vv, fa))))
        for i in span:
            out[i, at, :] = state[i]
            out[z.v + i, at, :] = back[i]


def arrange_kernel(z, levels, device, *refs):
    refs = list(refs)
    maps = [[refs.pop(0) for _ in range(2 * z.parts)] for _ in range(levels - 1)]
    vectors = [[refs.pop(0) for _ in range(2)] for _ in range(levels - 1)]
    for level in range(levels - 1):
        bit = (device[0] >> level) & 1
        for part in range(z.parts):
            own, other = maps[level][part], maps[level][z.parts + part]
            place_pair(bit, own, other, refs.pop(0), range(z.vv), range(z.vv, 3 * z.vv))
        own, other = vectors[level]
        place_pair(bit, own, other, refs.pop(0), range(z.v), range(z.v, 2 * z.v))


def final_kernel(z, levels, device, *refs):
    span = range(z.v)
    vv = z.vv
    refs = list(refs)

    def take(count):
        taken = refs[:count]
        del refs[:count]
        return taken

    arranged = [take(z.parts + 1) for _ in range(levels - 1)]
    responses = take(z.parts - 1)
    own_state, told, ops, driven, out, inside, stars = refs

    def load(base, at):
        return [inside[base + i, at, :] for i in span]

    half = (device[0] >> (levels - 1)) & 1
    for part in range(z.parts):
        at = pl.ds(part * z.chunk, z.chunk)
        word = [told[part * z.v + i] for i in span]
        g, base = (responses[part], 0) if part + 1 < z.parts else (told, z.parts * z.v)
        state = [own_state[i, at, :] for i in span]
        back = matvec(lambda i, j: g[base + i * z.v + j], state)
        for i in span:
            zero = jnp.zeros_like(word[i])
            inside[i, at, :] = jnp.where(half == 0, zero, word[i])
            inside[z.v + i, at, :] = jnp.where(half == 0, word[i] + back[i], zero)

    for level in range(levels - 2, -1, -1):
        bit = (device[0] >> level) & 1
        vectors = arranged[level][z.parts]
        for part in range(z.parts):
            at = pl.ds(part * z.chunk, z.chunk)
            fa, hb = [[vectors[k * z.v + i, at, :] for i in span] for k in range(2)]
            slots = arranged[level][part]

            def apply(base, vector):
                return matvec(lambda i, j: slots[base + i * z.v + j], vector)

            xa, yb = load(0, at), load(z.v, at)
            xb = plus(fa, apply(0, xa))
            ya = plus(plus(hb, apply(vv, xb)), apply(2 * vv, yb))
            for i in span:
                inside[i, at, :] = jnp.where(bit == 0, xa[i], xb[i])
                inside[z.v + i, at, :] = jnp.where(bit == 0, ya[i], yb[i])

    x = [inside[i] for i in span]
    y = [inside[z.v + i] for i in span]
    for r in range(z.rows):
        x = plus([driven[r, i] for i in span], matvec(lambda i, j: ops[r, i * z.v + j], x))
        for i in span:
            stars[r, i] = x[i]
    for r in range(z.rows - 1, -1, -1):
        y = plus(
            [stars[r, i] for i in span], matvec(lambda i, j: ops[r, vv + i * z.v + j], y)
        )
        for i in span:
            out[i, pl.ds(r, z.cells, stride=z.rows), :] = y[i]


def trig_tables(z):
    q = np.arange(z.width)[:, None]
    k = (np.arange(z.n)[:, None] + z.n * np.arange(z.per)[None, :]).reshape(1, z.n, 1, z.per)
    angle = 2 * np.pi * ((q.reshape(-1, 1, 1, 1) * k) % z.points) / z.points
    values = np.concatenate([np.cos(angle), np.sin(angle)], axis=2).reshape(z.width, -1)
    high = values.astype(np.float32).astype(ml_dtypes.bfloat16)
    low = (values - high.astype(np.float64)).astype(np.float32).astype(ml_dtypes.bfloat16)
    return high, low


def exchange(value, span, level, mirrored=False):
    flip = (2 << level) - 2 if mirrored else 1 << level
    return lax.ppermute(value, "span", [(d ^ flip, d) for d in range(span)])


def body(residual, inverse_diagonal, prior_increment, coupling, characteristic, cutoffs):
    pitch, span = lax.axis_size("pitch"), lax.axis_size("span")
    z = Sizes(residual, characteristic, pitch)
    vv = z.vv
    levels = span.bit_length() - 1
    residual_t = to_tiles(residual, z)
    prior_t = to_tiles(prior_increment, z)
    diag_t = to_tiles(inverse_diagonal, z)
    couple = jnp.transpose(coupling, (1, 0, 2))
    char = jnp.transpose(characteristic, (0, 3, 4, 1, 2)).reshape(-1, 2, z.harmonics)
    device = lax.axis_index("span").astype(jnp.int32).reshape(1)
    cell, part_cell = (z.cells, LANES), (z.chunk, LANES)
    field = (z.v, z.axial * z.block, LANES)
    scratch = pltpu.VMEM

    high, low = [jnp.asarray(table) for table in trig_tables(z)]
    cuts = cutoffs.reshape(1, 2)
    kept = [(char.shape, F32), (cuts.shape, jnp.int32), (high.shape, BF16), (low.shape, BF16)]
    ins = (couple, diag_t, prior_t, residual_t, char, cuts, high, low, device)
    residual_t, prior_t, couple, char, cuts, high, low, payload, ops, *maps = call(
        functools.partial(opening_kernel, z),
        [field, field, couple.shape, *kept, (z.planes + z.rows, LANES), (z.rows, 3 * vv) + cell]
        + [(3 * vv,) + part_cell] * z.parts,
        ins,
        [HBM] * 8 + [SMEM],
        [
            scratch((3 * vv,) + cell, F32),
            scratch((z.rows, vv) + cell, F32),
            scratch(diag_t.shape, F32),
            scratch((2 * vv,) + cell, F32),
            pltpu.SemaphoreType.DMA((z.v + 7,)),
        ],
        flops=10_000_000,
    )
    blocks = [payload]
    for j in range(1, pitch):
        pairs = [((e + j) % pitch, e) for e in range(pitch)]
        blocks.append(lax.ppermute(payload, "pitch", pairs))

    map_levels = []
    for level in range(levels - 1):
        others = []
        for value in maps:
            others.append(exchange(value, span, level))
        map_levels.append((maps, others))
        if level + 2 < levels:
            maps = [
                call(
                    functools.partial(merge_maps_kernel, z, level),
                    [(3 * vv,) + part_cell],
                    (device, mine, other),
                    [SMEM, VMEM, VMEM],
                    [scratch((6 * vv,) + part_cell, F32)],
                )[0]
                for mine, other in zip(maps, others)
            ]

    source, spec, splats = call(
        functools.partial(prepare_kernel, z),
        [field, (2, 2 * vv, z.harmonics), (2 * vv, z.rows, LANES)],
        (prior_t, residual_t, couple, char, cuts),
        [VMEM] * 5,
        flops=5_000_000,
    )

    rows = 2 * z.v * z.rows
    driven, vectors = call(
        functools.partial(spectral_kernel, z),
        [(z.rows, z.v) + cell, (2 * z.v,) + cell],
        (*blocks, high, low, spec, ops, source, splats),
        [VMEM] * (z.n + 6),
        [
            scratch((rows, z.harmonics), F32),
            scratch((rows, z.harmonics), F32),
            scratch(field, F32),
        ],
        flops=10_000_000,
    )

    vector_levels = []
    for level in range(levels - 1):
        other = exchange(vectors, span, level)
        vector_levels.append((vectors, other))
        mine, others = map_levels[level]
        ins = (device, *mine, *others, vectors, other)
        specs = [SMEM] + [VMEM] * (2 * z.parts + 2)
        if level + 2 < levels:
            vectors = call(
                functools.partial(merge_vectors_kernel, z, level),
                [(2 * z.v,) + cell],
                ins,
                specs,
                [scratch((3 * vv,) + part_cell, F32), scratch((4 * z.v,) + cell, F32)],
            )[0]
        else:
            tell, state = call(
                functools.partial(merge_last_kernel, z, level),
                [(z.parts * z.v + vv,) + part_cell, (z.v,) + cell],
                ins,
                specs,
                [scratch((5 * vv,) + part_cell, F32), scratch((4 * z.v,) + cell, F32)],
            )
    responses = []
    for part in range(z.parts - 1):
        given = [side[part] for side in map_levels[-1]]
        response = call(
            functools.partial(merge_response_kernel, z, levels - 2),
            [(vv,) + part_cell],
            (device, *given),
            [SMEM, VMEM, VMEM],
            [scratch((5 * vv,) + part_cell, F32)],
        )[0]
        responses.append(exchange(response, span, levels - 1, MIRRORED))
    told = exchange(tell, span, levels - 1, MIRRORED)

    arrays = []
    for mine, others in map_levels:
        arrays += [*mine, *others]
    for pair in vector_levels:
        arrays += pair
    shapes = [(3 * vv,) + part_cell] * z.parts + [(2 * z.v,) + cell]
    arrays = call(
        functools.partial(arrange_kernel, z, levels),
        shapes * (levels - 1),
        (device, *arrays),
        [SMEM] + [VMEM] * len(arrays),
    )
    arrays = [*arrays, *responses, state, told]
    update = call(
        functools.partial(final_kernel, z, levels),
        [field],
        (device, *arrays, ops, driven),
        [SMEM] + [VMEM] * (len(arrays) + 2),
        [
            scratch((2 * z.v,) + cell, F32),
            scratch((z.rows, z.v) + cell, F32),
        ],
        flops=2_000_000,
    )[0]
    return from_tiles(update, z)


def solution(mesh):
    in_specs = (
        P(None, None, "span", "pitch"),
        P(None, None, None, "span", "pitch"),
        P(None, None, "span", "pitch"),
        P(),
        P(),
        P(),
    )
    out_specs = P(None, None, "span", "pitch")
    return jax.shard_map(body, mesh=mesh, in_specs=in_specs, out_specs=out_specs, check_vma=False)
```
